32 devices in a mesh: kpt: 2 (over x), row: 8 (over z, y), col: 2 (over core).
Axes of the slice: x: 2, y: 2, z: 4, core: 2. Of those that a mesh axis runs over, the one named last changes fastest.
Arguments:
- wannier: float32 [64, 32, 1024], P('kpt', ('row', 'col')), parts along dimension 0, may hold values from -6 to 6
- pairs: int32 [384, 2], replicated, may hold values from 0 to 31, as said below
- gmap: int32 [8192], replicated, may hold values from 1 to 32767, as said below
- screened: bfloat16 [4, 2, 8192, 8192], P('kpt', None, 'row', 'col'), parts along dimension 0, may hold values from -0.046875 to 0.046875
Outputs:
- coulomb: float32 [2, 2, 768, 384], P(None, None, ('kpt', 'row', 'col')), parts along dimension 2
The draws below stay inside these ranges and needn't reach their ends.
There are 2 independent parts, one for each index of `kpt`. The reference program is written for one: setup_inputs(seed, part) draws one part's arguments, and reference() takes and returns one part's arrays. A program takes and returns all parts, laid end to end along the dimension named above; an argument that names none is the same for every part. Nothing has to cross between parts.
Inputs may be any that keep to these rules, and one draw needn't show every extreme that they name: `gmap`: 8192 distinct flat cells of the grid; cell 0 is never among them. `pairs`: in each row the first Wannier function is no greater than the second; no two rows are equal.
All inputs are finite; a program needn't handle non-finite values.
Results may differ from the reference program's by a relative error of at most 0.0082.
Values may be sent and summed in bfloat16 or wider, within the bound.
A program may use at most 128 MiB of HBM per device.

```python
import jax
import jax.numpy as jnp
from jax import lax

NW = 32
GX = 32
NG = 8192
NF = 2
NP = 384
GYZ = 1024


def draw_gmap(key, part):
    order = jax.random.permutation(key, GX * GX * GX - 1)
    return (order[:NG] + 1).astype(jnp.int32)


def draw_pairs(key, part):
    upper = jnp.triu_indices(NW)
    first_all = jnp.asarray(upper[0]).astype(jnp.int32)
    second_all = jnp.asarray(upper[1]).astype(jnp.int32)
    order = jax.random.permutation(jax.random.fold_in(key, 17), first_all.shape[0])
    chosen = order[:NP]
    return jnp.stack([first_all[chosen], second_all[chosen]], axis=1).astype(jnp.int32)


def block_scale(stream_key, dims, pieces, low, largest):
    level, own = 1.0, jax.random.fold_in(stream_key, 6)
    for position, blocks in pieces:
        draws = jnp.exp(jax.random.uniform(jax.random.fold_in(own, position), (blocks,), jnp.float32, low / len(pieces), largest / len(pieces)))
        level = level * jnp.repeat(draws, dims[position] // blocks).reshape([-1 if axis == position else 1 for axis in range(len(dims))])
    return level


def gaussian(own_key, shape, width, most, shards=(), dtype=jnp.bfloat16):
    values = width * jax.random.normal(own_key, shape, jnp.float32)
    if shards:
        values = values * block_scale(own_key, shape, shards, -0.22, 0.18)
    return jnp.clip(values, -most, most).astype(dtype)


def setup_inputs(seed: int = 0, part: int = 0) -> dict:
    streams_of = jax.random.split(jax.random.key(seed), 5)
    part_splits = jax.random.split(jax.random.fold_in(streams_of[4], part), 5)
    wannier = gaussian(part_splits[0], (NW, GX, GYZ), 1.0, 6.0, ((1, 16),), jnp.float32)
    pairs = draw_pairs(jax.random.fold_in(streams_of[4], 71), part)
    gmap = draw_gmap(jax.random.fold_in(streams_of[4], 71), part)
    screened = gaussian(part_splits[3], (NF, 2, NG, NG), (2 * NG) ** -0.5, 0.046875, ((2, 8), (3, 2)))
    return dict(wannier=wannier, pairs=pairs, gmap=gmap, screened=screened)


def reference(wannier, pairs, gmap, screened):
    grid = wannier.reshape(NW, GX, GX, GX)
    density = grid[pairs[:, 0]] * grid[pairs[:, 1]]
    spectrum = jnp.fft.fftn(density, axes=(1, 2, 3), norm='ortho').reshape(NP, GX * GX * GX)
    chosen = jnp.take(spectrum, gmap, axis=1)
    rho_real = jnp.real(chosen).astype(jnp.bfloat16)
    rho_imag = jnp.imag(chosen).astype(jnp.bfloat16)
    left_real = rho_real.astype(jnp.float32)
    left_imag = rho_imag.astype(jnp.float32)
    highest = lax.Precision.HIGHEST
    results = []
    for frequency in range(NF):
        w_real = screened[frequency, 0]
        w_imag = screened[frequency, 1]
        mixed_real = jnp.dot(w_real, rho_real.T, preferred_element_type=jnp.float32) - jnp.dot(w_imag, rho_imag.T, preferred_element_type=jnp.float32)
        mixed_imag = jnp.dot(w_real, rho_imag.T, preferred_element_type=jnp.float32) + jnp.dot(w_imag, rho_real.T, preferred_element_type=jnp.float32)
        u_real = jnp.dot(left_real, mixed_real, precision=highest) + jnp.dot(left_imag, mixed_imag, precision=highest)
        u_imag = jnp.dot(left_real, mixed_imag, precision=highest) - jnp.dot(left_imag, mixed_real, precision=highest)
        results.append(jnp.stack([u_real, u_imag], axis=0))
    return jnp.stack(results, axis=0) / jnp.sqrt(jnp.float32(NG))
```

```python
import functools
import math

import jax
import jax.numpy as jnp
import numpy as np
from jax import lax
from jax.experimental import pallas as pl
from jax.experimental.pallas import tpu as pltpu
from jax.sharding import PartitionSpec as P

LANES = 128
GROUP = 16
RADIX = 4
VMEM_BYTES = 66_000_000


def twiddle(re, im, c, s):
    if s == 0.0:
        return re, im
    if im is None:
        return re * c, re * (-s)
    if c == 0.0:
        return im * s, re * (-s)
    return re * c + im * s, im * c - re * s


def real_dft(xs):
    n = len(xs)
    if n == 1:
        return [(xs[0], None)]
    if n == 2:
        return [(xs[0] + xs[1], None), (xs[0] - xs[1], None)]
    even, odd = real_dft(xs[0::2]), real_dft(xs[1::2])
    out = [None] * (n // 2 + 1)
    for k in range(n // 4 + 1):
        er, ei = even[k]
        if 4 * k == n:
            c, s = 0.0, 1.0
        elif k == 0:
            c, s = 1.0, 0.0
        else:
            c, s = math.cos(2 * math.pi * k / n), math.sin(2 * math.pi * k / n)
        if c == 0.0 and odd[k][1] is None:
            tr, ti = None, odd[k][0] * -1.0
        else:
            tr, ti = twiddle(odd[k][0], odd[k][1], c, s)
        hi_r = er if tr is None else er + tr
        lo_r = er if tr is None else er - tr
        if ei is None and ti is None:
            hi_i = lo_i = None
        elif ei is None:
            hi_i, lo_i = ti, ti
        elif ti is None:
            hi_i, lo_i = ei, -ei
        else:
            hi_i, lo_i = ei + ti, ti - ei
        out[k] = (hi_r, hi_i)
        if n // 2 - k != k:
            out[n // 2 - k] = (lo_r, lo_i)
    return out


def rho_kernel(index_ref, sel_ref, grid_ref, table_ref, sign_ref, send_ref, own_ref, dens, mid, spec, *cells, parts=7):
    planes, _, area = grid_ref.shape
    own = sel_ref.shape[0] * GROUP // 2 // GROUP * 1
    chunks = sel_ref.shape[0] // (2 * GROUP)
    half = planes // 2 + 1
    inner = area // RADIX
    lanes = inner // LANES

    def fft(g, carry):
        r0 = pl.multiple_of(g * GROUP, GROUP)
        chosen = sel_ref[pl.ds(pl.multiple_of(g * 2 * GROUP, 2 * GROUP), 2 * GROUP), :]

        def plane(x, carry):
            both = jnp.dot(chosen, grid_ref[x], preferred_element_type=jnp.float32)
            dens[x] = both[:GROUP] * both[GROUP:]
            return carry

        lax.fori_loop(0, planes, plane, 0, unroll=True)

        def along_x(i, carry):
            n0 = pl.multiple_of((i // 2) * LANES, LANES)
            p0 = pl.multiple_of((i % 2) * 8, 8)
            terms = [dens[x, pl.ds(p0, 8), pl.ds(n0, LANES)] for x in range(planes)]
            for k, (re, im) in enumerate(real_dft(terms)):
                mid[k, 0, pl.ds(p0, 8), pl.ds(n0, LANES)] = re
                mid[k, 1, pl.ds(p0, 8), pl.ds(n0, LANES)] = jnp.zeros_like(re) if im is None else im
            return carry

        lax.fori_loop(0, 2 * area // LANES, along_x, 0)

        def along_y(k, carry):
            for l in range(lanes):
                at = [slice(t * inner + l * LANES, t * inner + (l + 1) * LANES) for t in range(RADIX)]
                a, b, c, d = [mid[k, 0, :, s] for s in at]
                e, f, g_, h = [mid[k, 1, :, s] for s in at]
                re = (a + c) + (b + d), (a - c) + (f - h), (a + c) - (b + d), (a - c) - (f - h)
                im = (e + g_) + (f + h), (e - g_) - (b - d), (e + g_) - (f + h), (e - g_) + (b - d)
                for q in range(RADIX):
                    lo, hi = slice(l * LANES, (l + 1) * LANES), slice(inner + l * LANES, inner + (l + 1) * LANES)
                    spec[k * RADIX + q, pl.ds(r0, GROUP), lo] = re[q].astype(jnp.bfloat16)
                    spec[k * RADIX + q, pl.ds(r0, GROUP), hi] = im[q].astype(jnp.bfloat16)
            return carry

        lax.fori_loop(0, half, along_y, 0)
        return carry

    if parts & 1:
        lax.fori_loop(0, chunks, fft, 0)

    def product(i, carry):
        nt = (((1,), (1,)), ((), ()))
        got = lax.dot_general(table_ref[i % RADIX], spec[i], nt, preferred_element_type=jnp.float32)
        at = pl.ds(pl.multiple_of(i * inner, inner), inner)
        re, im = got[:inner], got[inner:]
        cells[0][at, :] = re[:, :LANES]
        cells[1][at, :] = jnp.concatenate([re[:, LANES:], im[:, LANES:]], axis=1)
        cells[2][at, :] = im[:, :LANES]
        return carry

    if parts & 2:
        lax.fori_loop(0, half * RADIX, product, 0)
    rowid = lax.broadcasted_iota(jnp.int32, (8, LANES), 0)
    right = lax.broadcasted_iota(jnp.int32, (GROUP, LANES), 1) >= LANES // 2

    def picker(first, targets):
        def pick(i, carry):
            base = pl.multiple_of(i * GROUP, GROUP)
            from_ = pl.multiple_of(first + i * GROUP, GROUP)
            index = [index_ref[from_ + j] for j in range(GROUP)]
            sign = sign_ref[pl.ds(from_, GROUP), :]
            for t in range(3):
                halves = []
                for s in range(0, GROUP, 8):
                    got = jnp.broadcast_to(cells[t][pl.ds(index[s], 1), :], (8, LANES))
                    for j in range(1, 8):
                        got = jnp.where(rowid == j, jnp.broadcast_to(cells[t][pl.ds(index[s + j], 1), :], (8, LANES)), got)
                    halves.append(got)
                value = jnp.concatenate(halves, axis=0).astype(jnp.bfloat16)
                if t == 1:
                    value = jnp.where(right, value * sign, value)
                if t == 2:
                    value = value * sign
                for ref in targets:
                    ref[0][pl.ds(pl.multiple_of(ref[1] + base, GROUP), GROUP), t * LANES : (t + 1) * LANES] = value
            return carry

        return pick

    count, total = own_ref.shape[0], index_ref.shape[0]
    columns = total - count
    block = count - columns
    if parts & 4:
        lax.fori_loop(0, block // GROUP, picker(0, [(send_ref, 0), (own_ref, 0)]), 0)
        lax.fori_loop(0, columns // GROUP, picker(block, [(send_ref, block)]), 0)
        lax.fori_loop(0, columns // GROUP, picker(count, [(own_ref, block)]), 0)


def pair_coefficients(grid, table, sel, index, sign, columns, parts=7):
    planes, _, area = grid.shape
    own = sel.shape[0] // 2
    total = index.shape[0]
    count = total - columns
    half = planes // 2 + 1
    whole = pl.BlockSpec(memory_space=pltpu.VMEM)
    assert 2 * own == 3 * LANES
    return pl.pallas_call(
        functools.partial(rho_kernel, parts=parts),
        out_shape=[jax.ShapeDtypeStruct((count, 2 * own), jnp.bfloat16)] * 2,
        in_specs=[pl.BlockSpec(memory_space=pltpu.SMEM), whole, whole, whole, whole],
        out_specs=[whole, whole],
        scratch_shapes=[
            pltpu.VMEM((planes, GROUP, area), jnp.float32),
            pltpu.VMEM((half, 2, GROUP, area), jnp.float32),
            pltpu.VMEM((half * RADIX, own, 2 * area // RADIX), jnp.bfloat16),
        ]
        + [pltpu.VMEM((half * area, LANES), jnp.float32)] * 3,
        compiler_params=pltpu.CompilerParams(vmem_limit_bytes=VMEM_BYTES),
        cost_estimate=pl.CostEstimate(flops=10**10, bytes_accessed=8 * 1024 * 1024, transcendentals=0),
        name="rho",
    )(index, sel, grid, table, sign)


def element_kernel(scale, w_ref, own_ref, recv_ref, out_ref, right, turned, left, total):
    count, width = own_ref.shape
    freqs, parts, tile, columns = w_ref.shape
    block = count - columns
    i = pl.program_id(1)

    @pl.when((pl.program_id(0) == 0) & (i == 0))
    def _():
        col = lax.axis_index("col")
        flip = lax.broadcasted_iota(jnp.int32, (1, LANES), 1) < LANES // 2
        for ref, at in ((own_ref, col), (recv_ref, 1 - col)):
            at = pl.multiple_of(at * width, LANES)
            left[:, pl.ds(at, width)] = ref[:block]
            step = 256

            def turn(j, carry):
                src = pl.ds(pl.multiple_of(block + j * step, step), step)
                dst = pl.ds(pl.multiple_of(j * step, step), step)
                a, b, c = [ref[src, t * LANES : (t + 1) * LANES] for t in range(3)]
                right[dst, pl.ds(at, width)] = ref[src, :]
                turned[dst, pl.ds(at, LANES)] = -c
                rolled = pltpu.roll(b.astype(jnp.float32), LANES // 2, axis=1)
                turned[dst, pl.ds(pl.multiple_of(at + LANES, LANES), LANES)] = jnp.where(flip, -rolled, rolled).astype(b.dtype)
                turned[dst, pl.ds(pl.multiple_of(at + 2 * LANES, LANES), LANES)] = a
                return carry

            lax.fori_loop(0, columns // step, turn, 0)

    mixed = jnp.dot(w_ref[0, 0], right[...], preferred_element_type=jnp.float32)
    mixed += jnp.dot(w_ref[0, 1], turned[...], preferred_element_type=jnp.float32)
    mixed = (mixed * scale).astype(jnp.bfloat16)
    rows = left[pl.ds(pl.multiple_of(i * tile, tile), tile), :]
    got = lax.dot_general(rows, mixed, (((0,), (0,)), ((), ())), preferred_element_type=jnp.float32)

    @pl.when(i == 0)
    def _():
        total[...] = got

    @pl.when(i > 0)
    def _():
        total[...] += got

    @pl.when(i == pl.num_programs(1) - 1)
    def _():
        near = lax.broadcasted_iota(jnp.int32, (1, LANES), 1) < LANES // 2
        n, h = LANES, LANES // 2
        for o in range(2):
            for a0, p0, q0, size in ((0, 0, 2 * n, n), (n, n, n + h, h)):
                pr = slice(o * width + p0, o * width + p0 + size)
                qr = slice(o * width + q0, o * width + q0 + size)
                ar = slice(o * (width // 2) + a0, o * (width // 2) + a0 + size)
                for b in range(2):
                    s = [slice(b * width + t * n, b * width + (t + 1) * n) for t in range(3)]
                    out_ref[0, ar, s[0]] = (total[pr, s[0]] + total[qr, s[2]]).astype(out_ref.dtype)
                    out_ref[0, ar, s[2]] = (total[pr, s[2]] - total[qr, s[0]]).astype(out_ref.dtype)
                    rolled = pltpu.roll(total[qr, s[1]], h, axis=1)
                    out_ref[0, ar, s[1]] = (total[pr, s[1]] + jnp.where(near, rolled, -rolled)).astype(out_ref.dtype)


def matrix_elements(screened, own, recv, scale, tile=256):
    freqs, parts, rows, columns = screened.shape
    count, width = own.shape
    tile = min(tile, rows)
    whole = pl.BlockSpec(memory_space=pltpu.VMEM)
    return pl.pallas_call(
        functools.partial(element_kernel, scale),
        grid=(freqs, rows // tile),
        out_shape=jax.ShapeDtypeStruct((freqs, width, 2 * width), jnp.bfloat16),
        in_specs=[pl.BlockSpec((1, parts, tile, columns), lambda f, i: (f, 0, i, 0)), whole, whole],
        out_specs=pl.BlockSpec((1, width, 2 * width), lambda f, i: (f, 0, 0)),
        scratch_shapes=[
            pltpu.VMEM((columns, 2 * width), jnp.bfloat16),
            pltpu.VMEM((columns, 2 * width), jnp.bfloat16),
            pltpu.VMEM((rows, 2 * width), jnp.bfloat16),
            pltpu.VMEM((2 * width, 2 * width), jnp.float32),
        ],
        compiler_params=pltpu.CompilerParams(
            dimension_semantics=("arbitrary", "arbitrary"), vmem_limit_bytes=VMEM_BYTES
        ),
        cost_estimate=pl.CostEstimate(
            flops=8 * freqs * rows * columns * width, bytes_accessed=2 * screened.size, transcendentals=0
        ),
        name="elements",
    )(screened, own, recv)


def plane_table(area):
    side = math.isqrt(area)
    inner = area // RADIX
    q = np.arange(RADIX).reshape(-1, 1, 1)
    k, n = np.arange(inner).reshape(1, -1, 1), np.arange(inner).reshape(1, 1, -1)
    turn = (q + RADIX * (k // side)) * (n // side) + (k % side) * (n % side)
    angle = (turn % side) * (2.0 * math.pi / side)
    c, s = np.cos(angle), np.sin(angle)
    both = np.concatenate([np.concatenate([c, s], axis=2), np.concatenate([-s, c], axis=2)], axis=1)
    return jnp.asarray(both.astype(jnp.bfloat16))


def shards(wannier, pairs, gmap, screened):
    functions, _, area = wannier.shape
    side = math.isqrt(area)
    count = pairs.shape[0]
    columns = screened.shape[3]
    block = screened.shape[2]
    row, col = lax.axis_index("row"), lax.axis_index("col")
    cols = lax.axis_size("col")
    own = count // cols

    local = jnp.swapaxes(wannier, 0, 1).astype(jnp.bfloat16)
    grid = lax.all_gather(local, ("row", "col"), axis=0, tiled=True)
    depth = grid.shape[0]

    mine = lax.dynamic_slice_in_dim(pairs, col * own, own, 0)
    mine = mine.reshape(own // GROUP, GROUP, 2).swapaxes(1, 2).reshape(-1, 1)
    sel = (mine == jnp.arange(functions, dtype=jnp.int32)[None, :]).astype(jnp.bfloat16)

    flat = jnp.concatenate(
        [
            lax.dynamic_slice_in_dim(gmap, row * block, block, 0),
            lax.dynamic_slice_in_dim(gmap, (1 - col) * columns, columns, 0),
            lax.dynamic_slice_in_dim(gmap, col * columns, columns, 0),
        ]
    )
    kx, ky, kz = flat // area, (flat // side) % side, flat % side
    far = kx > depth // 2
    kx = jnp.where(far, depth - kx, kx)
    ky = jnp.where(far, (side - ky) % side, ky)
    kz = jnp.where(far, (side - kz) % side, kz)
    index = kx * area + (ky % RADIX) * (area // RADIX) + (ky // RADIX) * side + kz
    sign = jnp.broadcast_to(jnp.where(far, -1.0, 1.0).astype(jnp.bfloat16)[:, None], (flat.shape[0], LANES))

    send, keep = pair_coefficients(grid, plane_table(area), sel, index, sign, columns)
    swap = [(i, (i + 1) % cols) for i in range(cols)]
    recv = lax.ppermute(send, "col", swap)
    scale = 1.0 / (depth * area * math.sqrt(gmap.shape[0]))
    partial = matrix_elements(screened, keep, recv, scale)

    freqs = partial.shape[0]
    devices = lax.axis_size(("row", "col"))
    share = count // devices
    pieces = jnp.swapaxes(partial.reshape(freqs, devices, share, 2 * count), 0, 1)
    arrived = lax.all_to_all(pieces, ("row", "col"), split_axis=0, concat_axis=0, tiled=True)
    summed = jnp.sum(arrived.astype(jnp.float32), axis=0).reshape(freqs, share, cols, 3, 2, LANES // 2)
    real = jnp.concatenate([summed[:, :, :, 0].reshape(freqs, share, cols, LANES), summed[:, :, :, 1, 0]], axis=-1)
    imag = jnp.concatenate([summed[:, :, :, 2].reshape(freqs, share, cols, LANES), summed[:, :, :, 1, 1]], axis=-1)
    return jnp.stack([real.reshape(freqs, share, count), imag.reshape(freqs, share, count)], axis=1)


def solution(mesh):
    return jax.shard_map(
        shards,
        mesh=mesh,
        in_specs=(P("kpt", ("row", "col"), None), P(), P(), P("kpt", None, "row", "col")),
        out_specs=P(None, None, ("kpt", "row", "col"), None),
        check_vma=False,
    )
```

```python
import functools
import math

import jax
import jax.numpy as jnp
import numpy as np
from jax import lax
from jax.experimental import pallas as pl
from jax.experimental.pallas import tpu as pltpu
from jax.sharding import PartitionSpec as P

LANES = 128
GROUP = 16
RADIX = 4
TILES = 3
MESH = pl.DeviceIdType.MESH
VMEM_BYTES = 66_000_000


def twiddle(re, im, c, s):
    if s == 0.0:
        return re, im
    if im is None:
        return re * c, re * (-s)
    if c == 0.0:
        return im * s, re * (-s)
    return re * c + im * s, im * c - re * s


def real_dft(xs):
    n = len(xs)
    if n == 1:
        return [(xs[0], None)]
    if n == 2:
        return [(xs[0] + xs[1], None), (xs[0] - xs[1], None)]
    even, odd = real_dft(xs[0::2]), real_dft(xs[1::2])
    out = [None] * (n // 2 + 1)
    for k in range(n // 4 + 1):
        er, ei = even[k]
        if 4 * k == n:
            c, s = 0.0, 1.0
        elif k == 0:
            c, s = 1.0, 0.0
        else:
            c, s = math.cos(2 * math.pi * k / n), math.sin(2 * math.pi * k / n)
        if c == 0.0 and odd[k][1] is None:
            tr, ti = None, odd[k][0] * -1.0
        else:
            tr, ti = twiddle(odd[k][0], odd[k][1], c, s)
        hi_r = er if tr is None else er + tr
        lo_r = er if tr is None else er - tr
        if ei is None and ti is None:
            hi_i = lo_i = None
        elif ei is None:
            hi_i, lo_i = ti, ti
        elif ti is None:
            hi_i, lo_i = ei, -ei
        else:
            hi_i, lo_i = ei + ti, ti - ei
        out[k] = (hi_r, hi_i)
        if n // 2 - k != k:
            out[n // 2 - k] = (lo_r, lo_i)
    return out


def rho_kernel(index_ref, sel_ref, grid_ref, table_ref, send_ref, own_ref, dens, mid, spec, cells, parts=7):
    planes, _, area = grid_ref.shape
    chunks = sel_ref.shape[0] // (2 * GROUP)
    half = planes // 2 + 1
    inner = area // RADIX
    lanes = inner // LANES

    def fft(g, carry):
        r0 = pl.multiple_of(g * GROUP, GROUP)
        chosen = sel_ref[pl.ds(pl.multiple_of(g * 2 * GROUP, 2 * GROUP), 2 * GROUP), :]

        def plane(x, carry):
            both = jnp.dot(chosen, grid_ref[x], preferred_element_type=jnp.float32)
            dens[x] = both[:GROUP] * both[GROUP:]
            return carry

        lax.fori_loop(0, planes, plane, 0, unroll=True)

        def along_x(i, carry):
            n0 = pl.multiple_of((i // 2) * LANES, LANES)
            p0 = pl.multiple_of((i % 2) * 8, 8)
            terms = [dens[x, pl.ds(p0, 8), pl.ds(n0, LANES)] for x in range(planes)]
            for k, (re, im) in enumerate(real_dft(terms)):
                mid[k, 0, pl.ds(p0, 8), pl.ds(n0, LANES)] = re
                mid[k, 1, pl.ds(p0, 8), pl.ds(n0, LANES)] = jnp.zeros_like(re) if im is None else im
            return carry

        lax.fori_loop(0, 2 * area // LANES, along_x, 0)

        def along_y(k, carry):
            for l in range(lanes):
                at = [slice(t * inner + l * LANES, t * inner + (l + 1) * LANES) for t in range(RADIX)]
                a, b, c, d = [mid[k, 0, :, s] for s in at]
                e, f, g_, h = [mid[k, 1, :, s] for s in at]
                re = (a + c) + (b + d), (a - c) + (f - h), (a + c) - (b + d), (a - c) - (f - h)
                im = (e + g_) + (f + h), (e - g_) - (b - d), (e + g_) - (f + h), (e - g_) + (b - d)
                for q in range(RADIX):
                    lo, hi = slice(l * LANES, (l + 1) * LANES), slice(inner + l * LANES, inner + (l + 1) * LANES)
                    spec[k * RADIX + q, pl.ds(r0, GROUP), lo] = re[q].astype(jnp.bfloat16)
                    spec[k * RADIX + q, pl.ds(r0, GROUP), hi] = im[q].astype(jnp.bfloat16)
            return carry

        lax.fori_loop(0, half, along_y, 0)
        return carry

    if parts & 1:
        lax.fori_loop(0, chunks, fft, 0)

    def product(k, carry):
        nt = (((1,), (1,)), ((), ()))
        for q in range(RADIX):
            got = lax.dot_general(table_ref[q], spec[k * RADIX + q], nt, preferred_element_type=jnp.float32)
            re, im = got[:inner], got[inner:]
            three = re[:, :LANES], jnp.concatenate([re[:, LANES:], im[:, LANES:]], axis=1), im[:, :LANES]
            base = pl.multiple_of((k * RADIX + q) * inner * TILES, 8 * TILES)
            for t, value in enumerate(three):
                for j in range(inner // 8):
                    at = pl.multiple_of(base + (j * TILES + t) * 8, 8)
                    cells[pl.ds(at, 8), :] = value[j * 8 : (j + 1) * 8]
        return carry

    if parts & 2:
        lax.fori_loop(0, half, product, 0)
    rowid = lax.broadcasted_iota(jnp.int32, (8, LANES), 0)
    right = lax.broadcasted_iota(jnp.int32, (8, LANES), 1) >= LANES // 2
    count = own_ref.shape[0]
    total = index_ref.shape[0] * GROUP // (GROUP + 1)
    columns = total - count
    block = count - columns

    def picker(first, targets):
        def pick(i, carry):
            base = pl.multiple_of(i * GROUP, GROUP)
            from_ = pl.multiple_of(first + i * GROUP, GROUP)
            word = index_ref[total + first // GROUP + i]
            index = [index_ref[from_ + j] for j in range(GROUP)]
            halves = [[], [], []]
            for s in range(0, GROUP, 8):
                bits = lax.shift_right_logical(jnp.full((8, LANES), word, jnp.int32), rowid + s) & 1
                sign = 1.0 - 2.0 * bits.astype(jnp.float32)
                for t in range(TILES):
                    got = None
                    for j in range(8):
                        line = jnp.broadcast_to(cells[pl.ds(index[s + j] + 8 * t, 1), :], (8, LANES))
                        got = line if j == 0 else jnp.where(rowid == j, line, got)
                    if t == 1:
                        got = jnp.where(right, got * sign, got)
                    if t == 2:
                        got = got * sign
                    halves[t].append(got)
            for t in range(TILES):
                value = jnp.concatenate(halves[t], axis=0).astype(jnp.bfloat16)
                for ref, offset in targets:
                    at = pl.multiple_of(offset + base, GROUP)
                    ref[pl.ds(at, GROUP), t * LANES : (t + 1) * LANES] = value
            return carry

        return pick

    if parts & 4:
        lax.fori_loop(0, block // GROUP, picker(0, [(send_ref, 0), (own_ref, 0)]), 0)
        lax.fori_loop(0, columns // GROUP, picker(block, [(send_ref, block)]), 0)
        lax.fori_loop(0, columns // GROUP, picker(count, [(own_ref, block)]), 0)


def pair_coefficients(grid, table, sel, index, columns, parts=7):
    planes, _, area = grid.shape
    own = sel.shape[0] // 2
    total = index.shape[0] * GROUP // (GROUP + 1)
    count = total - columns
    half = planes // 2 + 1
    whole = pl.BlockSpec(memory_space=pltpu.VMEM)
    assert 2 * own == TILES * LANES
    return pl.pallas_call(
        functools.partial(rho_kernel, parts=parts),
        out_shape=[jax.ShapeDtypeStruct((count, 2 * own), jnp.bfloat16)] * 2,
        in_specs=[pl.BlockSpec(memory_space=pltpu.SMEM), whole, whole, whole],
        out_specs=[whole, whole],
        scratch_shapes=[
            pltpu.VMEM((planes, GROUP, area), jnp.float32),
            pltpu.VMEM((half, 2, GROUP, area), jnp.float32),
            pltpu.VMEM((half * RADIX, own, 2 * area // RADIX), jnp.bfloat16),
            pltpu.VMEM((half * area * TILES, LANES), jnp.float32),
        ],
        compiler_params=pltpu.CompilerParams(vmem_limit_bytes=VMEM_BYTES),
        cost_estimate=pl.CostEstimate(flops=10**10, bytes_accessed=8 * 1024 * 1024, transcendentals=0),
        name="rho",
    )(index, sel, grid, table)


def gather_kernel(x_ref, out_ref, zs, zr, ys, yr, cs, cr):
    row, col = lax.axis_index("row"), lax.axis_index("col")
    q, s = row // 2, row % 2
    lines = lax.axis_size("row") // 2
    peers = [lax.rem(q + d, lines) * 2 + s for d in range(1, lines)]
    pair, other = row + 1 - 2 * s, 1 - col
    barrier = pltpu.get_barrier_semaphore()
    for target in [{"row": p} for p in peers] + [{"row": pair}, {"col": other}]:
        pl.semaphore_signal(barrier, inc=1, device_id=target, device_id_type=MESH)
    pl.semaphore_wait(barrier, lines + 1)
    sent = []

    def send(src, r, c, target, ssem, rsem):
        copy = pltpu.make_async_remote_copy(
            src_ref=src, dst_ref=out_ref.at[r, c], send_sem=ssem, recv_sem=rsem, device_id=target, device_id_type=MESH
        )
        copy.start()
        sent.append(copy)

    def arrived(r, c, ssem, rsem):
        pltpu.make_async_remote_copy(
            src_ref=x_ref, dst_ref=out_ref.at[r, c], send_sem=ssem, recv_sem=rsem,
            device_id={"col": other}, device_id_type=MESH,
        ).wait_recv()

    send(x_ref, row, col, {"row": pair}, ys.at[0], yr.at[0])
    order = sorted(range(1, lines), key=lambda d: min(d, lines - d))
    for d in order:
        send(x_ref, row, col, {"row": peers[d - 1]}, zs.at[d - 1], zr.at[d - 1])
    send(x_ref, row, col, {"col": other}, cs.at[0], cr.at[0])
    out_ref[row, col] = x_ref[...]
    for d in order:
        r = lax.rem(q + lines - d, lines) * 2 + s
        arrived(r, col, zs.at[d - 1], zr.at[d - 1])
        send(out_ref.at[r, col], r, col, {"row": pair}, ys.at[d], yr.at[d])
        send(out_ref.at[r, col], r, col, {"col": other}, cs.at[d], cr.at[d])
    for d in [0] + order:
        r = lax.rem(q + lines - d, lines) * 2 + 1 - s
        arrived(r, col, ys.at[d], yr.at[d])
        send(out_ref.at[r, col], r, col, {"col": other}, cs.at[lines + d], cr.at[lines + d])
    for d in range(lines):
        r = lax.rem(q + lines - d, lines) * 2
        arrived(r + s, other, cs.at[d], cr.at[d])
        arrived(r + 1 - s, other, cs.at[lines + d], cr.at[lines + d])
    for copy in sent:
        copy.wait_send()


def gather_planes(local):
    rows, cols = lax.axis_size("row"), lax.axis_size("col")
    lines = rows // 2
    dma = pltpu.SemaphoreType.DMA
    whole = pl.BlockSpec(memory_space=pltpu.VMEM)
    got = pl.pallas_call(
        gather_kernel,
        out_shape=jax.ShapeDtypeStruct((rows, cols) + local.shape, local.dtype),
        in_specs=[whole],
        out_specs=whole,
        scratch_shapes=[dma((lines - 1,))] * 2 + [dma((lines,))] * 2 + [dma((2 * lines,))] * 2,
        compiler_params=pltpu.CompilerParams(collective_id=0, has_side_effects=True),
        name="planes",
    )(local)
    return got.reshape((-1,) + local.shape[1:])


def reduce_kernel(x_ref, out_ref, near, acc, far, ns, nr, fs, fr):
    rows = lax.axis_size("row")
    row, col = lax.axis_index("row"), lax.axis_index("col")
    other = 1 - col
    barrier = pltpu.get_barrier_semaphore()
    for target in [{"row": lax.rem(row + d, rows)} for d in range(1, rows)] + [{"col": other}]:
        pl.semaphore_signal(barrier, inc=1, device_id=target, device_id_type=MESH)
    pl.semaphore_wait(barrier, rows)
    order = sorted(range(rows), key=lambda d: -min(d, rows - d))
    first, second = [], {}
    for d in order:
        r = lax.rem(row + d, rows)
        copy = pltpu.make_async_remote_copy(
            src_ref=x_ref.at[r, other], dst_ref=near.at[d], send_sem=ns.at[d], recv_sem=nr.at[d],
            device_id={"col": other}, device_id_type=MESH,
        )
        copy.start()
        first.append(copy)
    for d, copy in zip(order, first):
        r = lax.rem(row + d, rows)
        copy.wait_recv()
        both = x_ref[r, col].astype(jnp.float32) + near[d].astype(jnp.float32)
        acc[d] = both.astype(acc.dtype)
        if d:
            second[d] = pltpu.make_async_remote_copy(
                src_ref=acc.at[d], dst_ref=far.at[d - 1], send_sem=fs.at[d - 1], recv_sem=fr.at[d - 1],
                device_id={"row": r}, device_id_type=MESH,
            )
            second[d].start()
    total = acc[0].astype(jnp.float32)
    for d in order[::-1][1:]:
        second[d].wait_recv()
        total += far[d - 1].astype(jnp.float32)
    half = LANES // 2
    width = total.shape[-1] // 2
    for b in range(2):
        x, y, z = [total[..., b * width + t * LANES : b * width + (t + 1) * LANES] for t in range(TILES)]
        for p, (big, small) in enumerate(((x, y[..., :half]), (z, y[..., half:]))):
            at = b * (width // 2)
            out_ref[:, p, :, at : at + LANES] = big
            out_ref[:, p, :, at + LANES : at + LANES + half] = small
    for copy in first + list(second.values()):
        copy.wait_send()


def reduce_elements(partial):
    rows, cols, freqs, share, width = partial.shape
    dma = pltpu.SemaphoreType.DMA
    whole = pl.BlockSpec(memory_space=pltpu.VMEM)
    piece = (freqs, share, width)
    return pl.pallas_call(
        reduce_kernel,
        out_shape=jax.ShapeDtypeStruct((freqs, 2, share, width // 2), jnp.float32),
        in_specs=[whole],
        out_specs=whole,
        scratch_shapes=[pltpu.VMEM((rows,) + piece, partial.dtype)] * 2
        + [pltpu.VMEM((rows - 1,) + piece, partial.dtype)]
        + [dma((rows,))] * 2
        + [dma((rows - 1,))] * 2,
        compiler_params=pltpu.CompilerParams(collective_id=1, has_side_effects=True),
        name="total",
    )(partial)


def element_kernel(scale, w_ref, own_ref, recv_ref, out_ref, right, turned, left, total, done):
    count, width = own_ref.shape
    freqs, parts, tile, columns = w_ref.shape
    block = count - columns
    i = pl.program_id(1)

    @pl.when((pl.program_id(0) == 0) & (i == 0))
    def _():
        col = lax.axis_index("col")
        flip = lax.broadcasted_iota(jnp.int32, (1, LANES), 1) < LANES // 2
        for ref, at in ((own_ref, col), (recv_ref, 1 - col)):
            at = pl.multiple_of(at * width, LANES)
            left[:, pl.ds(at, width)] = ref[:block]
            step = 256

            def turn(j, carry):
                src = pl.ds(pl.multiple_of(block + j * step, step), step)
                dst = pl.ds(pl.multiple_of(j * step, step), step)
                a, b, c = [ref[src, t * LANES : (t + 1) * LANES] for t in range(3)]
                right[dst, pl.ds(at, width)] = ref[src, :]
                turned[dst, pl.ds(at, LANES)] = -c
                rolled = pltpu.roll(b.astype(jnp.float32), LANES // 2, axis=1)
                turned[dst, pl.ds(pl.multiple_of(at + LANES, LANES), LANES)] = jnp.where(flip, -rolled, rolled).astype(b.dtype)
                turned[dst, pl.ds(pl.multiple_of(at + 2 * LANES, LANES), LANES)] = a
                return carry

            lax.fori_loop(0, columns // step, turn, 0)

    mixed = jnp.dot(w_ref[0, 0], right[...], preferred_element_type=jnp.float32)
    mixed += jnp.dot(w_ref[0, 1], turned[...], preferred_element_type=jnp.float32)
    mixed = (mixed * scale).astype(jnp.bfloat16)
    rows = left[pl.ds(pl.multiple_of(i * tile, tile), tile), :]
    got = lax.dot_general(rows, mixed, (((0,), (0,)), ((), ())), preferred_element_type=jnp.float32)

    @pl.when(i == 0)
    def _():
        total[...] = got

    @pl.when(i > 0)
    def _():
        total[...] += got

    @pl.when(i == pl.num_programs(1) - 1)
    def _():
        near = lax.broadcasted_iota(jnp.int32, (1, LANES), 1) < LANES // 2
        n, h = LANES, LANES // 2
        for o in range(2):
            for a0, p0, q0, size in ((0, 0, 2 * n, n), (n, n, n + h, h)):
                pr = slice(o * width + p0, o * width + p0 + size)
                qr = slice(o * width + q0, o * width + q0 + size)
                ar = slice(o * (width // 2) + a0, o * (width // 2) + a0 + size)
                for b in range(2):
                    s = [slice(b * width + t * n, b * width + (t + 1) * n) for t in range(3)]
                    x, z = total[pr, s[0]] + total[qr, s[2]], total[pr, s[2]] - total[qr, s[0]]
                    rolled = pltpu.roll(total[qr, s[1]], h, axis=1)
                    done[ar, s[0]], done[ar, s[2]] = x, z
                    done[ar, s[1]] = total[pr, s[1]] + jnp.where(near, rolled, -rolled)
        share = out_ref.shape[3]
        for r in range(out_ref.shape[0]):
            for c in range(out_ref.shape[1]):
                d = (r * out_ref.shape[1] + c) * share
                out_ref[r, c, 0] = done[d : d + share, :].astype(out_ref.dtype)


def matrix_elements(screened, own, recv, scale, tile=256):
    freqs, parts, rows, columns = screened.shape
    count, width = own.shape
    tile = min(tile, rows)
    members, cols = lax.axis_size("row"), lax.axis_size("col")
    share = width // (members * cols)
    whole = pl.BlockSpec(memory_space=pltpu.VMEM)
    return pl.pallas_call(
        functools.partial(element_kernel, scale),
        grid=(freqs, rows // tile),
        out_shape=jax.ShapeDtypeStruct((members, cols, freqs, share, 2 * width), jnp.bfloat16),
        in_specs=[pl.BlockSpec((1, parts, tile, columns), lambda f, i: (f, 0, i, 0)), whole, whole],
        out_specs=pl.BlockSpec((members, cols, 1, share, 2 * width), lambda f, i: (0, 0, f, 0, 0)),
        scratch_shapes=[
            pltpu.VMEM((columns, 2 * width), jnp.bfloat16),
            pltpu.VMEM((columns, 2 * width), jnp.bfloat16),
            pltpu.VMEM((rows, 2 * width), jnp.bfloat16),
            pltpu.VMEM((2 * width, 2 * width), jnp.float32),
            pltpu.VMEM((width, 2 * width), jnp.float32),
        ],
        compiler_params=pltpu.CompilerParams(
            dimension_semantics=("arbitrary", "arbitrary"), vmem_limit_bytes=VMEM_BYTES
        ),
        cost_estimate=pl.CostEstimate(
            flops=8 * freqs * rows * columns * width, bytes_accessed=2 * screened.size, transcendentals=0
        ),
        name="elements",
    )(screened, own, recv)


def plane_table(area):
    side = math.isqrt(area)
    inner = area // RADIX
    q = np.arange(RADIX).reshape(-1, 1, 1)
    k, n = np.arange(inner).reshape(1, -1, 1), np.arange(inner).reshape(1, 1, -1)
    turn = (q + RADIX * (k // side)) * (n // side) + (k % side) * (n % side)
    angle = (turn % side) * (2.0 * math.pi / side)
    c, s = np.cos(angle), np.sin(angle)
    both = np.concatenate([np.concatenate([c, s], axis=2), np.concatenate([-s, c], axis=2)], axis=1)
    return jnp.asarray(both.astype(jnp.bfloat16))


def shards(wannier, pairs, gmap, screened):
    functions, _, area = wannier.shape
    side = math.isqrt(area)
    count = pairs.shape[0]
    columns = screened.shape[3]
    block = screened.shape[2]
    row, col = lax.axis_index("row"), lax.axis_index("col")
    cols = lax.axis_size("col")
    own = count // cols

    local = jnp.swapaxes(wannier, 0, 1).astype(jnp.bfloat16)
    grid = gather_planes(local)
    depth = grid.shape[0]

    mine = lax.dynamic_slice_in_dim(pairs, col * own, own, 0)
    mine = mine.reshape(own // GROUP, GROUP, 2).swapaxes(1, 2).reshape(-1, 1)
    sel = (mine == jnp.arange(functions, dtype=jnp.int32)[None, :]).astype(jnp.bfloat16)

    flat = jnp.concatenate(
        [
            lax.dynamic_slice_in_dim(gmap, row * block, block, 0),
            lax.dynamic_slice_in_dim(gmap, (1 - col) * columns, columns, 0),
            lax.dynamic_slice_in_dim(gmap, col * columns, columns, 0),
        ]
    )
    kx, ky, kz = flat // area, (flat // side) % side, flat % side
    far = kx > depth // 2
    kx = jnp.where(far, depth - kx, kx)
    ky = jnp.where(far, (side - ky) % side, ky)
    kz = jnp.where(far, (side - kz) % side, kz)
    cell = kx * area + (ky % RADIX) * (area // RADIX) + (ky // RADIX) * side + kz
    bits = jnp.sum(far.astype(jnp.int32).reshape(-1, GROUP) << jnp.arange(GROUP, dtype=jnp.int32), axis=1)
    index = jnp.concatenate([(cell // 8) * (8 * TILES) + cell % 8, bits])

    send, keep = pair_coefficients(grid, plane_table(area), sel, index, columns)
    swap = [(i, (i + 1) % cols) for i in range(cols)]
    recv = lax.ppermute(send, "col", swap)
    scale = 1.0 / (depth * area * math.sqrt(gmap.shape[0]))
    partial = matrix_elements(screened, keep, recv, scale)

    return reduce_elements(partial)


def solution(mesh):
    return jax.shard_map(
        shards,
        mesh=mesh,
        in_specs=(P("kpt", ("row", "col"), None), P(), P(), P("kpt", None, "row", "col")),
        out_specs=P(None, None, ("kpt", "row", "col"), None),
        check_vma=False,
    )
```

```python
import functools
import math

import jax
import jax.numpy as jnp
import numpy as np
from jax import lax
from jax.experimental import pallas as pl
from jax.experimental.pallas import tpu as pltpu
from jax.sharding import PartitionSpec as P

LANES = 128
GROUP = 16
RADIX = 4
TILES = 3
PICK = 32
SENDS = 5
MESH = pl.DeviceIdType.MESH
VMEM_BYTES = 66_000_000


def twiddle(re, im, c, s):
    if s == 0.0:
        return re, im
    if im is None:
        return re * c, re * (-s)
    if c == 0.0:
        return im * s, re * (-s)
    return re * c + im * s, im * c - re * s


def real_dft(xs):
    n = len(xs)
    if n == 1:
        return [(xs[0], None)]
    if n == 2:
        return [(xs[0] + xs[1], None), (xs[0] - xs[1], None)]
    even, odd = real_dft(xs[0::2]), real_dft(xs[1::2])
    out = [None] * (n // 2 + 1)
    for k in range(n // 4 + 1):
        er, ei = even[k]
        if 4 * k == n:
            c, s = 0.0, 1.0
        elif k == 0:
            c, s = 1.0, 0.0
        else:
            c, s = math.cos(2 * math.pi * k / n), math.sin(2 * math.pi * k / n)
        if c == 0.0 and odd[k][1] is None:
            tr, ti = None, odd[k][0] * -1.0
        else:
            tr, ti = twiddle(odd[k][0], odd[k][1], c, s)
        hi_r = er if tr is None else er + tr
        lo_r = er if tr is None else er - tr
        if ei is None and ti is None:
            hi_i = lo_i = None
        elif ei is None:
            hi_i, lo_i = ti, ti
        elif ti is None:
            hi_i, lo_i = ei, -ei
        else:
            hi_i, lo_i = ei + ti, ti - ei
        out[k] = (hi_r, hi_i)
        if n // 2 - k != k:
            out[n // 2 - k] = (lo_r, lo_i)
    return out


def rho_kernel(index_ref, sel_ref, grid_ref, table_ref, own_ref, recv_ref, dens, mid, spec, cells, send_ref, ss, rs, parts=7):
    other = 1 - lax.axis_index("col")
    barrier = pltpu.get_barrier_semaphore()
    pl.semaphore_signal(barrier, inc=1, device_id={"col": other}, device_id_type=MESH)
    pl.semaphore_wait(barrier, 1)
    planes, _, area = grid_ref.shape
    chunks = sel_ref.shape[0] // (2 * GROUP)
    half = planes // 2 + 1
    inner = area // RADIX
    lanes = inner // LANES

    def fft(g, carry):
        r0 = pl.multiple_of(g * GROUP, GROUP)
        chosen = sel_ref[pl.ds(pl.multiple_of(g * 2 * GROUP, 2 * GROUP), 2 * GROUP), :]

        def plane(x, carry):
            both = jnp.dot(chosen, grid_ref[x], preferred_element_type=jnp.float32)
            dens[x] = both[:GROUP] * both[GROUP:]
            return carry

        lax.fori_loop(0, planes, plane, 0, unroll=True)

        def along_x(n, carry):
            n0 = pl.multiple_of(n * LANES, LANES)
            for p0 in range(0, GROUP, 8):
                terms = [dens[x, p0 : p0 + 8, pl.ds(n0, LANES)] for x in range(planes)]
                for k, (re, im) in enumerate(real_dft(terms)):
                    mid[k, 0, p0 : p0 + 8, pl.ds(n0, LANES)] = re
                    mid[k, 1, p0 : p0 + 8, pl.ds(n0, LANES)] = jnp.zeros_like(re) if im is None else im
            return carry

        lax.fori_loop(0, area // LANES, along_x, 0)

        def along_y(k, carry):
            for l in range(lanes):
                at = [slice(t * inner + l * LANES, t * inner + (l + 1) * LANES) for t in range(RADIX)]
                a, b, c, d = [mid[k, 0, :, s] for s in at]
                e, f, g_, h = [mid[k, 1, :, s] for s in at]
                re = (a + c) + (b + d), (a - c) + (f - h), (a + c) - (b + d), (a - c) - (f - h)
                im = (e + g_) + (f + h), (e - g_) - (b - d), (e + g_) - (f + h), (e - g_) + (b - d)
                for q in range(RADIX):
                    lo, hi = slice(l * LANES, (l + 1) * LANES), slice(inner + l * LANES, inner + (l + 1) * LANES)
                    spec[k * RADIX + q, pl.ds(r0, GROUP), lo] = re[q].astype(jnp.bfloat16)
                    spec[k * RADIX + q, pl.ds(r0, GROUP), hi] = im[q].astype(jnp.bfloat16)
            return carry

        lax.fori_loop(0, half, along_y, 0, unroll=True)
        return carry

    if parts & 1:
        lax.fori_loop(0, chunks, fft, 0)

    def product(k, carry):
        nt = (((1,), (1,)), ((), ()))
        for q in range(RADIX):
            got = lax.dot_general(table_ref[q], spec[k * RADIX + q], nt, preferred_element_type=jnp.float32)
            re, im = got[:inner], got[inner:]
            three = re[:, :LANES], jnp.concatenate([re[:, LANES:], im[:, LANES:]], axis=1), im[:, :LANES]
            base = pl.multiple_of((k * RADIX + q) * inner * TILES, 8 * TILES)
            for t, value in enumerate(three):
                for j in range(inner // 8):
                    at = pl.multiple_of(base + (j * TILES + t) * 8, 8)
                    cells[pl.ds(at, 8), :] = value[j * 8 : (j + 1) * 8]
        return carry

    if parts & 2:
        lax.fori_loop(0, half, product, 0)
    rowid = lax.broadcasted_iota(jnp.int32, (8, LANES), 0)
    right = lax.broadcasted_iota(jnp.int32, (8, LANES), 1) >= LANES // 2
    count = own_ref.shape[0]
    total = index_ref.shape[1] * PICK
    columns = total - count
    block = count - columns

    def picker(first, targets):
        def pick(i, carry):
            base = pl.multiple_of(i * PICK, PICK)
            trip = first // PICK + i
            word = index_ref[PICK, trip]
            index = [index_ref[j, trip] for j in range(PICK)]
            halves = [[], [], []]
            for s in range(0, PICK, 8):
                bits = lax.shift_right_logical(jnp.full((8, LANES), word, jnp.int32), rowid + s) & 1
                sign = 1.0 - 2.0 * bits.astype(jnp.float32)
                for t in range(TILES):
                    got = None
                    for j in range(8):
                        line = jnp.broadcast_to(cells[pl.ds(index[s + j] + 8 * t, 1), :], (8, LANES))
                        got = line if j == 0 else jnp.where(rowid == j, line, got)
                    if t == 1:
                        got = jnp.where(right, got * sign, got)
                    if t == 2:
                        got = got * sign
                    halves[t].append(got)
            for t in range(TILES):
                value = jnp.concatenate(halves[t], axis=0).astype(jnp.bfloat16)
                for ref, offset in targets:
                    at = pl.multiple_of(offset + base, PICK)
                    ref[pl.ds(at, PICK), t * LANES : (t + 1) * LANES] = value
            return carry

        return pick

    sent = []

    def send(first, size):
        at = pl.ds(first, size)
        copy = pltpu.make_async_remote_copy(
            src_ref=send_ref.at[at], dst_ref=recv_ref.at[at], send_sem=ss.at[len(sent)], recv_sem=rs.at[len(sent)],
            device_id={"col": other}, device_id_type=MESH,
        )
        copy.start()
        sent.append(copy)

    lax.fori_loop(0, block // PICK, picker(0, [(send_ref, 0), (own_ref, 0)]), 0)
    send(0, block)
    piece = columns // (SENDS - 1)
    for n in range(SENDS - 1):
        first = block + n * piece
        lax.fori_loop(0, piece // PICK, picker(first, [(send_ref, first)]), 0)
        send(first, piece)
    lax.fori_loop(0, columns // PICK, picker(count, [(own_ref, block)]), 0)
    for copy in sent:
        copy.wait()


def pair_coefficients(grid, table, sel, index, columns, parts=7):
    planes, _, area = grid.shape
    own = sel.shape[0] // 2
    total = index.shape[1] * PICK
    count = total - columns
    half = planes // 2 + 1
    whole = pl.BlockSpec(memory_space=pltpu.VMEM)
    assert 2 * own == TILES * LANES
    return pl.pallas_call(
        functools.partial(rho_kernel, parts=parts),
        out_shape=[jax.ShapeDtypeStruct((count, 2 * own), jnp.bfloat16)] * 2,
        in_specs=[pl.BlockSpec(memory_space=pltpu.SMEM), whole, whole, whole],
        out_specs=[whole, whole],
        scratch_shapes=[
            pltpu.VMEM((planes, GROUP, area), jnp.float32),
            pltpu.VMEM((half, 2, GROUP, area), jnp.float32),
            pltpu.VMEM((half * RADIX, own, 2 * area // RADIX), jnp.bfloat16),
            pltpu.VMEM((half * area * TILES, LANES), jnp.float32),
            pltpu.VMEM((count, 2 * own), jnp.bfloat16),
            pltpu.SemaphoreType.DMA((SENDS,)),
            pltpu.SemaphoreType.DMA((SENDS,)),
        ],
        compiler_params=pltpu.CompilerParams(vmem_limit_bytes=VMEM_BYTES, collective_id=2, has_side_effects=True),
        cost_estimate=pl.CostEstimate(flops=10**10, bytes_accessed=8 * 1024 * 1024, transcendentals=0),
        name="rho",
    )(index, sel, grid, table)


def gather_kernel(x_ref, out_ref, zs, zr, ys, yr, cs, cr):
    row, col = lax.axis_index("row"), lax.axis_index("col")
    q, s = row // 2, row % 2
    lines = lax.axis_size("row") // 2
    peers = [lax.rem(q + d, lines) * 2 + s for d in range(1, lines)]
    pair, other = row + 1 - 2 * s, 1 - col
    barrier = pltpu.get_barrier_semaphore()
    for target in [{"row": p} for p in peers] + [{"row": pair}, {"col": other}]:
        pl.semaphore_signal(barrier, inc=1, device_id=target, device_id_type=MESH)
    pl.semaphore_wait(barrier, lines + 1)
    sent = []

    def send(src, r, c, target, ssem, rsem):
        copy = pltpu.make_async_remote_copy(
            src_ref=src, dst_ref=out_ref.at[r, c], send_sem=ssem, recv_sem=rsem, device_id=target, device_id_type=MESH
        )
        copy.start()
        sent.append(copy)

    def arrived(r, c, ssem, rsem):
        pltpu.make_async_remote_copy(
            src_ref=x_ref, dst_ref=out_ref.at[r, c], send_sem=ssem, recv_sem=rsem,
            device_id={"col": other}, device_id_type=MESH,
        ).wait_recv()

    send(x_ref, row, col, {"row": pair}, ys.at[0], yr.at[0])
    order = sorted(range(1, lines), key=lambda d: min(d, lines - d))
    for d in order:
        send(x_ref, row, col, {"row": peers[d - 1]}, zs.at[d - 1], zr.at[d - 1])
    send(x_ref, row, col, {"col": other}, cs.at[0], cr.at[0])
    out_ref[row, col] = x_ref[...]
    for d in order:
        r = lax.rem(q + lines - d, lines) * 2 + s
        arrived(r, col, zs.at[d - 1], zr.at[d - 1])
        send(out_ref.at[r, col], r, col, {"row": pair}, ys.at[d], yr.at[d])
        send(out_ref.at[r, col], r, col, {"col": other}, cs.at[d], cr.at[d])
    for d in [0] + order:
        r = lax.rem(q + lines - d, lines) * 2 + 1 - s
        arrived(r, col, ys.at[d], yr.at[d])
        send(out_ref.at[r, col], r, col, {"col": other}, cs.at[lines + d], cr.at[lines + d])
    for d in range(lines):
        r = lax.rem(q + lines - d, lines) * 2
        arrived(r + s, other, cs.at[d], cr.at[d])
        arrived(r + 1 - s, other, cs.at[lines + d], cr.at[lines + d])
    for copy in sent:
        copy.wait_send()


def gather_planes(local):
    rows, cols = lax.axis_size("row"), lax.axis_size("col")
    lines = rows // 2
    dma = pltpu.SemaphoreType.DMA
    whole = pl.BlockSpec(memory_space=pltpu.VMEM)
    got = pl.pallas_call(
        gather_kernel,
        out_shape=jax.ShapeDtypeStruct((rows, cols) + local.shape, local.dtype),
        in_specs=[whole],
        out_specs=whole,
        scratch_shapes=[dma((lines - 1,))] * 2 + [dma((lines,))] * 2 + [dma((2 * lines,))] * 2,
        compiler_params=pltpu.CompilerParams(collective_id=0, has_side_effects=True),
        name="planes",
    )(local)
    return got.reshape((-1,) + local.shape[1:])


def element_kernel(
    scale, w_ref, own_ref, recv_ref, out_ref, right, turned, left, total, done, part, near, both, far, ns, nr, fs, fr
):
    count, width = own_ref.shape
    _, parts, tile, columns = w_ref.shape
    block = count - columns
    which, i = pl.program_id(0), pl.program_id(1)
    freqs = part.shape[0]
    rows = lax.axis_size("row")
    row, col = lax.axis_index("row"), lax.axis_index("col")
    other = 1 - col

    def to_pair(f):
        return pltpu.make_async_remote_copy(
            src_ref=part.at[f, other], dst_ref=near.at[f], send_sem=ns.at[f], recv_sem=nr.at[f],
            device_id={"col": other}, device_id_type=MESH,
        )

    def to_row(f, d):
        return pltpu.make_async_remote_copy(
            src_ref=both.at[f, d], dst_ref=far.at[f, d - 1], send_sem=fs.at[f, d - 1], recv_sem=fr.at[f, d - 1],
            device_id={"row": lax.rem(row + d, rows)}, device_id_type=MESH,
        )

    order = sorted(range(1, rows), key=lambda d: -min(d, rows - d))

    def pass_on(f):
        to_pair(f).wait_recv()
        for d in order + [0]:
            r = lax.rem(row + d, rows)
            both[f, d] = (part[f, col, r].astype(jnp.float32) + near[f, r].astype(jnp.float32)).astype(both.dtype)
        for d in order:
            to_row(f, d).start()

    @pl.when((which == 0) & (i == 0))
    def _():
        barrier = pltpu.get_barrier_semaphore()
        for target in [{"row": lax.rem(row + d, rows)} for d in range(1, rows)] + [{"col": other}]:
            pl.semaphore_signal(barrier, inc=1, device_id=target, device_id_type=MESH)
        pl.semaphore_wait(barrier, rows)
        flip = lax.broadcasted_iota(jnp.int32, (1, LANES), 1) < LANES // 2
        for ref, at in ((own_ref, col), (recv_ref, other)):
            at = pl.multiple_of(at * width, LANES)
            left[:, pl.ds(at, width)] = ref[:block]
            step = 256

            def turn(j, carry):
                src = pl.ds(pl.multiple_of(block + j * step, step), step)
                dst = pl.ds(pl.multiple_of(j * step, step), step)
                a, b, c = [ref[src, t * LANES : (t + 1) * LANES] for t in range(3)]
                right[dst, pl.ds(at, width)] = ref[src, :]
                turned[dst, pl.ds(at, LANES)] = -c
                rolled = pltpu.roll(b.astype(jnp.float32), LANES // 2, axis=1)
                turned[dst, pl.ds(pl.multiple_of(at + LANES, LANES), LANES)] = jnp.where(flip, -rolled, rolled).astype(b.dtype)
                turned[dst, pl.ds(pl.multiple_of(at + 2 * LANES, LANES), LANES)] = a
                return carry

            lax.fori_loop(0, columns // step, turn, 0)

    mixed = jnp.dot(w_ref[0, 0], right[...], preferred_element_type=jnp.float32)
    mixed += jnp.dot(w_ref[0, 1], turned[...], preferred_element_type=jnp.float32)
    mixed = (mixed * scale).astype(jnp.bfloat16)
    mine = left[pl.ds(pl.multiple_of(i * tile, tile), tile), :]
    got = lax.dot_general(mine, mixed, (((0,), (0,)), ((), ())), preferred_element_type=jnp.float32)

    @pl.when(i == 0)
    def _():
        total[...] = got

    @pl.when(i > 0)
    def _():
        total[...] += got

    @pl.when(i == pl.num_programs(1) - 1)
    def _():
        low = lax.broadcasted_iota(jnp.int32, (1, LANES), 1) < LANES // 2
        n, h = LANES, LANES // 2
        for o in range(2):
            for a0, p0, q0, size in ((0, 0, 2 * n, n), (n, n, n + h, h)):
                pr = slice(o * width + p0, o * width + p0 + size)
                qr = slice(o * width + q0, o * width + q0 + size)
                ar = slice(o * (width // 2) + a0, o * (width // 2) + a0 + size)
                for b in range(2):
                    s = [slice(b * width + t * n, b * width + (t + 1) * n) for t in range(3)]
                    x, z = total[pr, s[0]] + total[qr, s[2]], total[pr, s[2]] - total[qr, s[0]]
                    rolled = pltpu.roll(total[qr, s[1]], h, axis=1)
                    done[ar, s[0]], done[ar, s[2]] = x, z
                    done[ar, s[1]] = total[pr, s[1]] + jnp.where(low, rolled, -rolled)
        share = part.shape[3]
        for f in range(freqs):

            @pl.when(which == f)
            def _():
                for r in range(part.shape[2]):
                    for c in range(part.shape[1]):
                        d = (r * part.shape[1] + c) * share
                        part[f, c, r] = done[d : d + share, :].astype(part.dtype)
                to_pair(f).start()

    for f in range(freqs - 1):

        @pl.when((which == f + 1) & (i == 0))
        def _():
            pass_on(f)

    @pl.when((which == freqs - 1) & (i == pl.num_programs(1) - 1))
    def _():
        pass_on(freqs - 1)
        h = LANES // 2
        for f in range(freqs):
            summed = both[f, 0].astype(jnp.float32)
            for d in order[::-1]:
                to_row(f, d).wait_recv()
                summed += far[f, d - 1].astype(jnp.float32)
            for b in range(2):
                x, y, z = [summed[:, b * width + t * LANES : b * width + (t + 1) * LANES] for t in range(TILES)]
                for p, (big, small) in enumerate(((x, y[:, :h]), (z, y[:, h:]))):
                    at = b * (width // 2)
                    out_ref[f, p, :, at : at + LANES] = big
                    out_ref[f, p, :, at + LANES : at + LANES + h] = small
        for f in range(freqs):
            to_pair(f).wait_send()
            for d in order:
                to_row(f, d).wait_send()


def matrix_elements(screened, own, recv, scale, tile=256):
    freqs, parts, rows, columns = screened.shape
    count, width = own.shape
    tile = min(tile, rows)
    members, cols = lax.axis_size("row"), lax.axis_size("col")
    share = width // (members * cols)
    dma = pltpu.SemaphoreType.DMA
    whole = pl.BlockSpec(memory_space=pltpu.VMEM)
    return pl.pallas_call(
        functools.partial(element_kernel, scale),
        grid=(freqs, rows // tile),
        out_shape=jax.ShapeDtypeStruct((freqs, 2, share, width), jnp.float32),
        in_specs=[pl.BlockSpec((1, parts, tile, columns), lambda f, i: (f, 0, i, 0)), whole, whole],
        out_specs=pl.BlockSpec((freqs, 2, share, width), lambda f, i: (0, 0, 0, 0)),
        scratch_shapes=[
            pltpu.VMEM((columns, 2 * width), jnp.bfloat16),
            pltpu.VMEM((columns, 2 * width), jnp.bfloat16),
            pltpu.VMEM((rows, 2 * width), jnp.bfloat16),
            pltpu.VMEM((2 * width, 2 * width), jnp.float32),
            pltpu.VMEM((width, 2 * width), jnp.float32),
            pltpu.VMEM((freqs, cols, members, share, 2 * width), jnp.bfloat16),
            pltpu.VMEM((freqs, members, share, 2 * width), jnp.bfloat16),
            pltpu.VMEM((freqs, members, share, 2 * width), jnp.bfloat16),
            pltpu.VMEM((freqs, members - 1, share, 2 * width), jnp.bfloat16),
            dma((freqs,)),
            dma((freqs,)),
            dma((freqs, members - 1)),
            dma((freqs, members - 1)),
        ],
        compiler_params=pltpu.CompilerParams(
            dimension_semantics=("arbitrary", "arbitrary"),
            vmem_limit_bytes=VMEM_BYTES,
            collective_id=1,
            has_side_effects=True,
        ),
        cost_estimate=pl.CostEstimate(
            flops=8 * freqs * rows * columns * width, bytes_accessed=2 * screened.size, transcendentals=0
        ),
        name="elements",
    )(screened, own, recv)


def plane_table(area):
    side = math.isqrt(area)
    inner = area // RADIX
    q = np.arange(RADIX).reshape(-1, 1, 1)
    k, n = np.arange(inner).reshape(1, -1, 1), np.arange(inner).reshape(1, 1, -1)
    turn = (q + RADIX * (k // side)) * (n // side) + (k % side) * (n % side)
    angle = (turn % side) * (2.0 * math.pi / side)
    c, s = np.cos(angle), np.sin(angle)
    both = np.concatenate([np.concatenate([c, s], axis=2), np.concatenate([-s, c], axis=2)], axis=1)
    return jnp.asarray(both.astype(jnp.bfloat16))


def shards(wannier, pairs, gmap, screened):
    functions, _, area = wannier.shape
    side = math.isqrt(area)
    count = pairs.shape[0]
    columns = screened.shape[3]
    block = screened.shape[2]
    row, col = lax.axis_index("row"), lax.axis_index("col")
    cols = lax.axis_size("col")
    own = count // cols

    local = jnp.swapaxes(wannier, 0, 1).astype(jnp.bfloat16)
    grid = gather_planes(local)
    depth = grid.shape[0]

    mine = lax.dynamic_slice_in_dim(pairs, col * own, own, 0)
    mine = mine.reshape(own // GROUP, GROUP, 2).swapaxes(1, 2).reshape(-1, 1)
    sel = (mine == jnp.arange(functions, dtype=jnp.int32)[None, :]).astype(jnp.bfloat16)

    flat = jnp.concatenate(
        [
            lax.dynamic_slice_in_dim(gmap, row * block, block, 0),
            lax.dynamic_slice_in_dim(gmap, (1 - col) * columns, columns, 0),
            lax.dynamic_slice_in_dim(gmap, col * columns, columns, 0),
        ]
    )
    kx, ky, kz = flat // area, (flat // side) % side, flat % side
    far = kx > depth // 2
    kx = jnp.where(far, depth - kx, kx)
    ky = jnp.where(far, (side - ky) % side, ky)
    kz = jnp.where(far, (side - kz) % side, kz)
    cell = kx * area + (ky % RADIX) * (area // RADIX) + (ky // RADIX) * side + kz
    bits = jnp.sum(far.astype(jnp.int32).reshape(-1, PICK) << jnp.arange(PICK, dtype=jnp.int32), axis=1)
    index = jnp.concatenate([((cell // 8) * (8 * TILES) + cell % 8).reshape(-1, PICK).T, bits[None, :]], axis=0)

    keep, recv = pair_coefficients(grid, plane_table(area), sel, index, columns)
    scale = 1.0 / (depth * area * math.sqrt(gmap.shape[0]))
    return matrix_elements(screened, keep, recv, scale)


def solution(mesh):
    return jax.shard_map(
        shards,
        mesh=mesh,
        in_specs=(P("kpt", ("row", "col"), None), P(), P(), P("kpt", None, "row", "col")),
        out_specs=P(None, None, ("kpt", "row", "col"), None),
        check_vma=False,
    )
```

```python
import functools
import math

import jax
import jax.numpy as jnp
import numpy as np
from jax import lax
from jax.experimental import pallas as pl
from jax.experimental.pallas import tpu as pltpu
from jax.sharding import PartitionSpec as P

LANES = 128
GROUP = 16
RADIX = 4
TILES = 3
PICK = 32
SENDS = 5
MESH = pl.DeviceIdType.MESH
VMEM_BYTES = 66_000_000


def twiddle(re, im, c, s):
    if s == 0.0:
        return re, im
    if im is None:
        return re * c, re * (-s)
    if c == 0.0:
        return im * s, re * (-s)
    return re * c + im * s, im * c - re * s


def real_dft(xs):
    n = len(xs)
    if n == 1:
        return [(xs[0], None)]
    if n == 2:
        return [(xs[0] + xs[1], None), (xs[0] - xs[1], None)]
    even, odd = real_dft(xs[0::2]), real_dft(xs[1::2])
    out = [None] * (n // 2 + 1)
    for k in range(n // 4 + 1):
        er, ei = even[k]
        if 4 * k == n:
            c, s = 0.0, 1.0
        elif k == 0:
            c, s = 1.0, 0.0
        else:
            c, s = math.cos(2 * math.pi * k / n), math.sin(2 * math.pi * k / n)
        if c == 0.0 and odd[k][1] is None:
            tr, ti = None, odd[k][0] * -1.0
        else:
            tr, ti = twiddle(odd[k][0], odd[k][1], c, s)
        hi_r = er if tr is None else er + tr
        lo_r = er if tr is None else er - tr
        if ei is None and ti is None:
            hi_i = lo_i = None
        elif ei is None:
            hi_i, lo_i = ti, ti
        elif ti is None:
            hi_i, lo_i = ei, -ei
        else:
            hi_i, lo_i = ei + ti, ti - ei
        out[k] = (hi_r, hi_i)
        if n // 2 - k != k:
            out[n // 2 - k] = (lo_r, lo_i)
    return out


def rho_kernel(index_ref, sel_ref, grid_ref, table_ref, out_ref, dens, mid, spec, cells, send_ref, ss, rs, ids, *index):
    col = lax.axis_index("col")
    other = 1 - col
    loads = [pltpu.make_async_copy(index_ref.at[j], index[j], ids.at[j]) for j in range(len(index))]
    for load in loads:
        load.start()
    barrier = pltpu.get_barrier_semaphore()
    pl.semaphore_signal(barrier, inc=1, device_id={"col": other}, device_id_type=MESH)
    pl.semaphore_wait(barrier, 1)
    planes, _, area = grid_ref.shape
    chunks = sel_ref.shape[0] // (2 * GROUP)
    half = planes // 2 + 1
    inner = area // RADIX
    lanes = inner // LANES

    def fft(g, carry):
        r0 = pl.multiple_of(g * GROUP, GROUP)
        chosen = sel_ref[pl.ds(pl.multiple_of(g * 2 * GROUP, 2 * GROUP), 2 * GROUP), :]

        def plane(x, carry):
            both = jnp.dot(chosen, grid_ref[x], preferred_element_type=jnp.float32)
            dens[x] = both[:GROUP] * both[GROUP:]
            return carry

        lax.fori_loop(0, planes, plane, 0, unroll=True)

        def along_x(n, carry):
            n0 = pl.multiple_of(n * LANES, LANES)
            for p0 in range(0, GROUP, 8):
                terms = [dens[x, p0 : p0 + 8, pl.ds(n0, LANES)] for x in range(planes)]
                for k, (re, im) in enumerate(real_dft(terms)):
                    mid[k, 0, p0 : p0 + 8, pl.ds(n0, LANES)] = re
                    mid[k, 1, p0 : p0 + 8, pl.ds(n0, LANES)] = jnp.zeros_like(re) if im is None else im
            return carry

        lax.fori_loop(0, area // LANES, along_x, 0)

        def along_y(k, carry):
            for l in range(lanes):
                at = [slice(t * inner + l * LANES, t * inner + (l + 1) * LANES) for t in range(RADIX)]
                a, b, c, d = [mid[k, 0, :, s] for s in at]
                e, f, g_, h = [mid[k, 1, :, s] for s in at]
                re = (a + c) + (b + d), (a - c) + (f - h), (a + c) - (b + d), (a - c) - (f - h)
                im = (e + g_) + (f + h), (e - g_) - (b - d), (e + g_) - (f + h), (e - g_) + (b - d)
                for q in range(RADIX):
                    lo, hi = slice(l * LANES, (l + 1) * LANES), slice(inner + l * LANES, inner + (l + 1) * LANES)
                    spec[k * RADIX + q, pl.ds(r0, GROUP), lo] = re[q].astype(jnp.bfloat16)
                    spec[k * RADIX + q, pl.ds(r0, GROUP), hi] = im[q].astype(jnp.bfloat16)
            return carry

        lax.fori_loop(0, half, along_y, 0, unroll=True)
        return carry

    lax.fori_loop(0, chunks, fft, 0)

    def product(k, carry):
        nt = (((1,), (1,)), ((), ()))
        for q in range(RADIX):
            got = lax.dot_general(table_ref[q], spec[k * RADIX + q], nt, preferred_element_type=jnp.float32)
            re, im = got[:inner], got[inner:]
            three = re[:, :LANES], jnp.concatenate([re[:, LANES:], im[:, LANES:]], axis=1), im[:, :LANES]
            base = pl.multiple_of((k * RADIX + q) * inner * TILES, 8 * TILES)
            for t, value in enumerate(three):
                for j in range(inner // 8):
                    at = pl.multiple_of(base + (j * TILES + t) * 8, 8)
                    cells[pl.ds(at, 8), :] = value[j * 8 : (j + 1) * 8]
        return carry

    lax.fori_loop(0, half, product, 0)
    rowid = lax.broadcasted_iota(jnp.int32, (8, LANES), 0)
    right = lax.broadcasted_iota(jnp.int32, (8, LANES), 1) >= LANES // 2
    count, width = send_ref.shape
    total = index_ref.shape[2] * 8
    columns = total - count
    block = count - columns
    lane = pl.multiple_of(col * width, LANES)
    for load in loads:
        load.wait()

    def picker(first, targets):
        def pick(i, carry):
            base = pl.multiple_of(i * PICK, PICK)
            trip = first // PICK + i
            word = index[8][0, trip]
            octets = [trip * (PICK // 8) + m for m in range(PICK // 8)]
            at_cell = [index[j][0, m] for m in octets for j in range(8)]
            halves = [[], [], []]
            for s in range(0, PICK, 8):
                bits = lax.shift_right_logical(jnp.full((8, LANES), word, jnp.int32), rowid + s) & 1
                sign = 1.0 - 2.0 * bits.astype(jnp.float32)
                for t in range(TILES):
                    got = None
                    for j in range(8):
                        line = jnp.broadcast_to(cells[pl.ds(at_cell[s + j] + 8 * t, 1), :], (8, LANES))
                        got = line if j == 0 else jnp.where(rowid == j, line, got)
                    if t == 1:
                        got = jnp.where(right, got * sign, got)
                    if t == 2:
                        got = got * sign
                    halves[t].append(got)
            for t in range(TILES):
                value = jnp.concatenate(halves[t], axis=0).astype(jnp.bfloat16)
                for ref, offset, across in targets:
                    at = pl.multiple_of(offset + base, PICK)
                    ref[pl.ds(at, PICK), pl.ds(pl.multiple_of(across + t * LANES, LANES), LANES)] = value
            return carry

        return pick

    sent = []

    def send(first, size):
        at = pl.ds(first, size)
        copy = pltpu.make_async_remote_copy(
            src_ref=send_ref.at[at], dst_ref=out_ref.at[at, pl.ds(lane, width)], send_sem=ss.at[len(sent)], recv_sem=rs.at[len(sent)],
            device_id={"col": other}, device_id_type=MESH,
        )
        copy.start()
        sent.append(copy)

    lax.fori_loop(0, block // PICK, picker(0, [(send_ref, 0, 0), (out_ref, 0, lane)]), 0)
    send(0, block)
    piece = columns // (SENDS - 1)
    for n in range(SENDS - 1):
        first = block + n * piece
        lax.fori_loop(0, piece // PICK, picker(first, [(send_ref, first, 0)]), 0)
        send(first, piece)
    lax.fori_loop(0, columns // PICK, picker(count, [(out_ref, block, lane)]), 0)
    for copy in sent:
        copy.wait()


def pair_coefficients(grid, table, sel, index, columns):
    planes, _, area = grid.shape
    own = sel.shape[0] // 2
    total = index.shape[2] * 8
    count = total - columns
    half = planes // 2 + 1
    whole = pl.BlockSpec(memory_space=pltpu.VMEM)
    assert 2 * own == TILES * LANES
    return pl.pallas_call(
        rho_kernel,
        out_shape=jax.ShapeDtypeStruct((count, 4 * own), jnp.bfloat16),
        in_specs=[pl.BlockSpec(memory_space=pl.ANY), whole, whole, whole],
        out_specs=whole,
        scratch_shapes=[
            pltpu.VMEM((planes, GROUP, area), jnp.float32),
            pltpu.VMEM((half, 2, GROUP, area), jnp.float32),
            pltpu.VMEM((half * RADIX, own, 2 * area // RADIX), jnp.bfloat16),
            pltpu.VMEM((half * area * TILES, LANES), jnp.float32),
            pltpu.VMEM((count, 2 * own), jnp.bfloat16),
            pltpu.SemaphoreType.DMA((SENDS,)),
            pltpu.SemaphoreType.DMA((SENDS,)),
            pltpu.SemaphoreType.DMA((9,)),
        ]
        + [pltpu.SMEM((1, index.shape[2]), jnp.int32)] * 9,
        compiler_params=pltpu.CompilerParams(vmem_limit_bytes=VMEM_BYTES, collective_id=2, has_side_effects=True),
        cost_estimate=pl.CostEstimate(flops=10**10, bytes_accessed=8 * 1024 * 1024, transcendentals=0),
        name="rho",
    )(index, sel, grid, table)


def gather_kernel(x_ref, out_ref, zs, zr, ys, yr, cs, cr):
    row, col = lax.axis_index("row"), lax.axis_index("col")
    q, s = row // 2, row % 2
    lines = lax.axis_size("row") // 2
    peers = [lax.rem(q + d, lines) * 2 + s for d in range(1, lines)]
    pair, other = row + 1 - 2 * s, 1 - col
    barrier = pltpu.get_barrier_semaphore()
    for target in [{"row": p} for p in peers] + [{"row": pair}, {"col": other}]:
        pl.semaphore_signal(barrier, inc=1, device_id=target, device_id_type=MESH)
    pl.semaphore_wait(barrier, lines + 1)
    sent = []

    def send(src, r, c, target, ssem, rsem):
        copy = pltpu.make_async_remote_copy(
            src_ref=src, dst_ref=out_ref.at[r, c], send_sem=ssem, recv_sem=rsem, device_id=target, device_id_type=MESH
        )
        copy.start()
        sent.append(copy)

    def arrived(r, c, ssem, rsem):
        pltpu.make_async_remote_copy(
            src_ref=x_ref, dst_ref=out_ref.at[r, c], send_sem=ssem, recv_sem=rsem,
            device_id={"col": other}, device_id_type=MESH,
        ).wait_recv()

    send(x_ref, row, col, {"row": pair}, ys.at[0], yr.at[0])
    order = sorted(range(1, lines), key=lambda d: min(d, lines - d))
    for d in order:
        send(x_ref, row, col, {"row": peers[d - 1]}, zs.at[d - 1], zr.at[d - 1])
    send(x_ref, row, col, {"col": other}, cs.at[0], cr.at[0])
    out_ref[row, col] = x_ref[...]
    for d in order:
        r = lax.rem(q + lines - d, lines) * 2 + s
        arrived(r, col, zs.at[d - 1], zr.at[d - 1])
        send(out_ref.at[r, col], r, col, {"row": pair}, ys.at[d], yr.at[d])
        send(out_ref.at[r, col], r, col, {"col": other}, cs.at[d], cr.at[d])
    for d in [0] + order:
        r = lax.rem(q + lines - d, lines) * 2 + 1 - s
        arrived(r, col, ys.at[d], yr.at[d])
        send(out_ref.at[r, col], r, col, {"col": other}, cs.at[lines + d], cr.at[lines + d])
    for d in range(lines):
        r = lax.rem(q + lines - d, lines) * 2
        arrived(r + s, other, cs.at[d], cr.at[d])
        arrived(r + 1 - s, other, cs.at[lines + d], cr.at[lines + d])
    for copy in sent:
        copy.wait_send()


def gather_planes(local):
    rows, cols = lax.axis_size("row"), lax.axis_size("col")
    lines = rows // 2
    dma = pltpu.SemaphoreType.DMA
    whole = pl.BlockSpec(memory_space=pltpu.VMEM)
    got = pl.pallas_call(
        gather_kernel,
        out_shape=jax.ShapeDtypeStruct((rows, cols) + local.shape, local.dtype),
        in_specs=[whole],
        out_specs=whole,
        scratch_shapes=[dma((lines - 1,))] * 2 + [dma((lines,))] * 2 + [dma((2 * lines,))] * 2,
        compiler_params=pltpu.CompilerParams(collective_id=0, has_side_effects=True),
        name="planes",
    )(local)
    return got.reshape((-1,) + local.shape[1:])


def element_kernel(
    scale, w_ref, right_ref, out_ref, mixed, total, done, part, near, both, far, ns, nr, fs, fr
):
    count, width = right_ref.shape[0], right_ref.shape[1] // 2
    _, parts, tile, columns = w_ref.shape
    block = count - columns
    which, i = pl.program_id(0), pl.program_id(1)
    freqs = part.shape[0]
    rows = lax.axis_size("row")
    row, col = lax.axis_index("row"), lax.axis_index("col")
    other = 1 - col

    def to_pair(f):
        return pltpu.make_async_remote_copy(
            src_ref=part.at[f, other], dst_ref=near.at[f], send_sem=ns.at[f], recv_sem=nr.at[f],
            device_id={"col": other}, device_id_type=MESH,
        )

    def to_row(f, d):
        return pltpu.make_async_remote_copy(
            src_ref=both.at[f, d], dst_ref=far.at[f, d - 1], send_sem=fs.at[f, d - 1], recv_sem=fr.at[f, d - 1],
            device_id={"row": lax.rem(row + d, rows)}, device_id_type=MESH,
        )

    order = sorted(range(1, rows), key=lambda d: -min(d, rows - d))

    def pass_on(f):
        to_pair(f).wait_recv()
        for d in order + [0]:
            r = lax.rem(row + d, rows)
            both[f, d] = (part[f, col, r].astype(jnp.float32) + near[f, r].astype(jnp.float32)).astype(both.dtype)
        for d in order:
            to_row(f, d).start()

    @pl.when((which == 0) & (i == 0))
    def _():
        barrier = pltpu.get_barrier_semaphore()
        for target in [{"row": lax.rem(row + d, rows)} for d in range(1, rows)] + [{"col": other}]:
            pl.semaphore_signal(barrier, inc=1, device_id=target, device_id_type=MESH)
        pl.semaphore_wait(barrier, rows)
        flip = lax.broadcasted_iota(jnp.int32, (1, LANES), 1) < LANES // 2

    real = jnp.dot(w_ref[0, 0], right_ref[block:, :], preferred_element_type=jnp.float32)
    imag = jnp.dot(w_ref[0, 1], right_ref[block:, :], preferred_element_type=jnp.float32)
    low = lax.broadcasted_iota(jnp.int32, (1, LANES), 1) < LANES // 2
    where = pl.ds(pl.multiple_of(i * tile, tile), tile)
    for b in range(2):
        s = [slice(b * width + t * LANES, b * width + (t + 1) * LANES) for t in range(TILES)]
        rolled = pltpu.roll(imag[:, s[1]], LANES // 2, axis=1)
        turned = -imag[:, s[2]], jnp.where(low, -rolled, rolled), imag[:, s[0]]
        for t in range(TILES):
            mixed[where, s[t]] = ((real[:, s[t]] + turned[t]) * scale).astype(mixed.dtype)

    @pl.when(i == pl.num_programs(1) - 1)
    def _():
        total[...] = lax.dot_general(
            right_ref[:block, :], mixed[...], (((0,), (0,)), ((), ())), preferred_element_type=jnp.float32
        )
        n, h = LANES, LANES // 2
        for o in range(2):
            for a0, p0, q0, size in ((0, 0, 2 * n, n), (n, n, n + h, h)):
                pr = slice(o * width + p0, o * width + p0 + size)
                qr = slice(o * width + q0, o * width + q0 + size)
                ar = slice(o * (width // 2) + a0, o * (width // 2) + a0 + size)
                for b in range(2):
                    s = [slice(b * width + t * n, b * width + (t + 1) * n) for t in range(3)]
                    x, z = total[pr, s[0]] + total[qr, s[2]], total[pr, s[2]] - total[qr, s[0]]
                    rolled = pltpu.roll(total[qr, s[1]], h, axis=1)
                    done[ar, s[0]], done[ar, s[2]] = x, z
                    done[ar, s[1]] = total[pr, s[1]] + jnp.where(low, rolled, -rolled)
        share = part.shape[3]
        for f in range(freqs):

            @pl.when(which == f)
            def _():
                for r in range(part.shape[2]):
                    for c in range(part.shape[1]):
                        d = (r * part.shape[1] + c) * share
                        part[f, c, r] = done[d : d + share, :].astype(part.dtype)
                to_pair(f).start()

    for f in range(freqs - 1):

        @pl.when((which == f + 1) & (i == 0))
        def _():
            pass_on(f)

    @pl.when((which == freqs - 1) & (i == pl.num_programs(1) - 1))
    def _():
        pass_on(freqs - 1)
        h = LANES // 2
        for f in range(freqs):
            summed = both[f, 0].astype(jnp.float32)
            for d in order[::-1]:
                to_row(f, d).wait_recv()
                summed += far[f, d - 1].astype(jnp.float32)
            for b in range(2):
                x, y, z = [summed[:, b * width + t * LANES : b * width + (t + 1) * LANES] for t in range(TILES)]
                for p, (big, small) in enumerate(((x, y[:, :h]), (z, y[:, h:]))):
                    at = b * (width // 2)
                    out_ref[f, p, :, at : at + LANES] = big
                    out_ref[f, p, :, at + LANES : at + LANES + h] = small
        for f in range(freqs):
            to_pair(f).wait_send()
            for d in order:
                to_row(f, d).wait_send()


def matrix_elements(screened, right, scale, tile=256):
    freqs, parts, rows, columns = screened.shape
    count, width = right.shape[0], right.shape[1] // 2
    tile = min(tile, rows)
    members, cols = lax.axis_size("row"), lax.axis_size("col")
    share = width // (members * cols)
    dma = pltpu.SemaphoreType.DMA
    whole = pl.BlockSpec(memory_space=pltpu.VMEM)
    return pl.pallas_call(
        functools.partial(element_kernel, scale),
        grid=(freqs, rows // tile),
        out_shape=jax.ShapeDtypeStruct((freqs, 2, share, width), jnp.float32),
        in_specs=[pl.BlockSpec((1, parts, tile, columns), lambda f, i: (f, 0, i, 0)), whole],
        out_specs=pl.BlockSpec((freqs, 2, share, width), lambda f, i: (0, 0, 0, 0)),
        scratch_shapes=[
            pltpu.VMEM((rows, 2 * width), jnp.bfloat16),
            pltpu.VMEM((2 * width, 2 * width), jnp.float32),
            pltpu.VMEM((width, 2 * width), jnp.float32),
            pltpu.VMEM((freqs, cols, members, share, 2 * width), jnp.bfloat16),
            pltpu.VMEM((freqs, members, share, 2 * width), jnp.bfloat16),
            pltpu.VMEM((freqs, members, share, 2 * width), jnp.bfloat16),
            pltpu.VMEM((freqs, members - 1, share, 2 * width), jnp.bfloat16),
            dma((freqs,)),
            dma((freqs,)),
            dma((freqs, members - 1)),
            dma((freqs, members - 1)),
        ],
        compiler_params=pltpu.CompilerParams(
            dimension_semantics=("arbitrary", "arbitrary"),
            vmem_limit_bytes=VMEM_BYTES,
            collective_id=1,
            has_side_effects=True,
        ),
        cost_estimate=pl.CostEstimate(
            flops=8 * freqs * rows * columns * width, bytes_accessed=2 * screened.size, transcendentals=0
        ),
        name="elements",
    )(screened, right)


def plane_table(area):
    side = math.isqrt(area)
    inner = area // RADIX
    q = np.arange(RADIX).reshape(-1, 1, 1)
    k, n = np.arange(inner).reshape(1, -1, 1), np.arange(inner).reshape(1, 1, -1)
    turn = (q + RADIX * (k // side)) * (n // side) + (k % side) * (n % side)
    angle = (turn % side) * (2.0 * math.pi / side)
    c, s = np.cos(angle), np.sin(angle)
    both = np.concatenate([np.concatenate([c, s], axis=2), np.concatenate([-s, c], axis=2)], axis=1)
    return jnp.asarray(both.astype(jnp.bfloat16))


def shards(wannier, pairs, gmap, screened):
    functions, _, area = wannier.shape
    side = math.isqrt(area)
    count = pairs.shape[0]
    columns = screened.shape[3]
    block = screened.shape[2]
    row, col = lax.axis_index("row"), lax.axis_index("col")
    cols = lax.axis_size("col")
    own = count // cols

    local = jnp.swapaxes(wannier, 0, 1).astype(jnp.bfloat16)
    grid = gather_planes(local)
    depth = grid.shape[0]

    mine = lax.dynamic_slice_in_dim(pairs, col * own, own, 0)
    mine = mine.reshape(own // GROUP, GROUP, 2).swapaxes(1, 2).reshape(-1, 1)
    sel = (mine == jnp.arange(functions, dtype=jnp.int32)[None, :]).astype(jnp.bfloat16)

    flat = jnp.concatenate(
        [
            lax.dynamic_slice_in_dim(gmap, row * block, block, 0),
            lax.dynamic_slice_in_dim(gmap, (1 - col) * columns, columns, 0),
            lax.dynamic_slice_in_dim(gmap, col * columns, columns, 0),
        ]
    )
    kx, ky, kz = flat // area, (flat // side) % side, flat % side
    far = kx > depth // 2
    kx = jnp.where(far, depth - kx, kx)
    ky = jnp.where(far, (side - ky) % side, ky)
    kz = jnp.where(far, (side - kz) % side, kz)
    cell = kx * area + (ky % RADIX) * (area // RADIX) + (ky // RADIX) * side + kz
    bits = jnp.sum(far.astype(jnp.int32).reshape(-1, PICK) << jnp.arange(PICK, dtype=jnp.int32), axis=1)
    bits = jnp.pad(bits, (0, cell.shape[0] // 8 - bits.shape[0]))
    index = jnp.concatenate([((cell // 8) * (8 * TILES) + cell % 8).reshape(-1, 8).T, bits[None, :]], axis=0)[:, None, :]

    right = pair_coefficients(grid, plane_table(area), sel, index, columns)
    scale = 1.0 / (depth * area * math.sqrt(gmap.shape[0]))
    return matrix_elements(screened, right, scale)


def solution(mesh):
    return jax.shard_map(
        shards,
        mesh=mesh,
        in_specs=(P("kpt", ("row", "col"), None), P(), P(), P("kpt", None, "row", "col")),
        out_specs=P(None, None, ("kpt", "row", "col"), None),
        check_vma=False,
    )
```

```python
import functools
import math

import jax
import jax.numpy as jnp
import numpy as np
from jax import lax
from jax.experimental import pallas as pl
from jax.experimental.pallas import tpu as pltpu
from jax.sharding import PartitionSpec as P

LANES = 128
GROUP = 16
RADIX = 4
TILES = 3
PICK = 32
TILE = 512
SENDS = 5
MESH = pl.DeviceIdType.MESH
VMEM_BYTES = 66_000_000
ELEMENT_BYTES = 66_000_000


def twiddle(re, im, c, s):
    if s == 0.0:
        return re, im
    if im is None:
        return re * c, re * (-s)
    if c == 0.0:
        return im * s, re * (-s)
    return re * c + im * s, im * c - re * s


def real_dft(xs):
    n = len(xs)
    if n == 1:
        return [(xs[0], None)]
    if n == 2:
        return [(xs[0] + xs[1], None), (xs[0] - xs[1], None)]
    even, odd = real_dft(xs[0::2]), real_dft(xs[1::2])
    out = [None] * (n // 2 + 1)
    for k in range(n // 4 + 1):
        er, ei = even[k]
        if 4 * k == n:
            c, s = 0.0, 1.0
        elif k == 0:
            c, s = 1.0, 0.0
        else:
            c, s = math.cos(2 * math.pi * k / n), math.sin(2 * math.pi * k / n)
        if c == 0.0 and odd[k][1] is None:
            tr, ti = None, odd[k][0] * -1.0
        else:
            tr, ti = twiddle(odd[k][0], odd[k][1], c, s)
        hi_r = er if tr is None else er + tr
        lo_r = er if tr is None else er - tr
        if ei is None and ti is None:
            hi_i = lo_i = None
        elif ei is None:
            hi_i, lo_i = ti, ti
        elif ti is None:
            hi_i, lo_i = ei, -ei
        else:
            hi_i, lo_i = ei + ti, ti - ei
        out[k] = (hi_r, hi_i)
        if n // 2 - k != k:
            out[n // 2 - k] = (lo_r, lo_i)
    return out


def rho_kernel(index_ref, sel_ref, grid_ref, table_ref, out_ref, dens, mid, spec, cells, send_ref, ss, rs, ids, *index):
    col = lax.axis_index("col")
    other = 1 - col
    loads = [pltpu.make_async_copy(index_ref.at[j], index[j], ids.at[j]) for j in range(len(index))]
    for load in loads:
        load.start()
    barrier = pltpu.get_barrier_semaphore()
    pl.semaphore_signal(barrier, inc=1, device_id={"col": other}, device_id_type=MESH)
    pl.semaphore_wait(barrier, 1)
    planes, _, area = grid_ref.shape
    chunks = sel_ref.shape[0] // (2 * GROUP)
    half = planes // 2 + 1
    inner = area // RADIX
    lanes = inner // LANES

    def fft(g, carry):
        r0 = pl.multiple_of(g * GROUP, GROUP)
        chosen = sel_ref[pl.ds(pl.multiple_of(g * 2 * GROUP, 2 * GROUP), 2 * GROUP), :]

        def plane(x, carry):
            both = jnp.dot(chosen, grid_ref[x], preferred_element_type=jnp.float32)
            dens[x] = both[:GROUP] * both[GROUP:]
            return carry

        lax.fori_loop(0, planes, plane, 0, unroll=True)

        def along_x(n, carry):
            n0 = pl.multiple_of(n * LANES, LANES)
            for p0 in range(0, GROUP, 8):
                terms = [dens[x, p0 : p0 + 8, pl.ds(n0, LANES)] for x in range(planes)]
                for k, (re, im) in enumerate(real_dft(terms)):
                    mid[k, 0, p0 : p0 + 8, pl.ds(n0, LANES)] = re
                    mid[k, 1, p0 : p0 + 8, pl.ds(n0, LANES)] = jnp.zeros_like(re) if im is None else im
            return carry

        lax.fori_loop(0, area // LANES, along_x, 0)

        def along_y(k, carry):
            for l in range(lanes):
                at = [slice(t * inner + l * LANES, t * inner + (l + 1) * LANES) for t in range(RADIX)]
                a, b, c, d = [mid[k, 0, :, s] for s in at]
                e, f, g_, h = [mid[k, 1, :, s] for s in at]
                re = (a + c) + (b + d), (a - c) + (f - h), (a + c) - (b + d), (a - c) - (f - h)
                im = (e + g_) + (f + h), (e - g_) - (b - d), (e + g_) - (f + h), (e - g_) + (b - d)
                for q in range(RADIX):
                    lo, hi = slice(l * LANES, (l + 1) * LANES), slice(inner + l * LANES, inner + (l + 1) * LANES)
                    spec[k * RADIX + q, pl.ds(r0, GROUP), lo] = re[q].astype(jnp.bfloat16)
                    spec[k * RADIX + q, pl.ds(r0, GROUP), hi] = im[q].astype(jnp.bfloat16)
            return carry

        lax.fori_loop(0, half, along_y, 0, unroll=True)
        return carry

    lax.fori_loop(0, chunks, fft, 0)

    def product(k, carry):
        nt = (((1,), (1,)), ((), ()))
        for q in range(RADIX):
            got = lax.dot_general(table_ref[q], spec[k * RADIX + q], nt, preferred_element_type=jnp.float32)
            re, im = got[:inner], got[inner:]
            three = re[:, :LANES], jnp.concatenate([re[:, LANES:], im[:, LANES:]], axis=1), im[:, :LANES]
            base = pl.multiple_of((k * RADIX + q) * inner * TILES, 8 * TILES)
            for t, value in enumerate(three):
                for j in range(inner // 8):
                    at = pl.multiple_of(base + (j * TILES + t) * 8, 8)
                    cells[pl.ds(at, 8), :] = value[j * 8 : (j + 1) * 8]
        return carry

    lax.fori_loop(0, half, product, 0)
    rowid = lax.broadcasted_iota(jnp.int32, (8, LANES), 0)
    right = lax.broadcasted_iota(jnp.int32, (8, LANES), 1) >= LANES // 2
    count, width = send_ref.shape
    total = index_ref.shape[2] * 8
    columns = total - count
    block = count - columns
    pair_lane = pl.multiple_of(col * 2 * LANES, LANES)
    rest_lane = pl.multiple_of((4 + col) * LANES, LANES)
    kept = pair_lane, rest_lane, pair_lane + LANES
    for load in loads:
        load.wait()

    def picker(first, targets):
        def pick(i, carry):
            base = pl.multiple_of(i * PICK, PICK)
            trip = first // PICK + i
            word = index[8][0, trip]
            octets = [trip * (PICK // 8) + m for m in range(PICK // 8)]
            at_cell = [index[j][0, m] for m in octets for j in range(8)]
            halves = [[], [], []]
            for s in range(0, PICK, 8):
                bits = lax.shift_right_logical(jnp.full((8, LANES), word, jnp.int32), rowid + s) & 1
                sign = 1.0 - 2.0 * bits.astype(jnp.float32)
                for t in range(TILES):
                    got = None
                    for j in range(8):
                        line = jnp.broadcast_to(cells[pl.ds(at_cell[s + j] + 8 * t, 1), :], (8, LANES))
                        got = line if j == 0 else jnp.where(rowid == j, line, got)
                    if t == 1:
                        got = jnp.where(right, got * sign, got)
                    if t == 2:
                        got = got * sign
                    halves[t].append(got)
            for t in range(TILES):
                value = jnp.concatenate(halves[t], axis=0).astype(jnp.bfloat16)
                for ref, offset, across in targets:
                    at = pl.multiple_of(offset + base, PICK)
                    ref[pl.ds(at, PICK), pl.ds(pl.multiple_of(across[t], LANES), LANES)] = value
            return carry

        return pick

    sent = []

    def send(first, size):
        at = pl.ds(first, size)
        for lane, start, span in ((pair_lane, 0, 2 * LANES), (rest_lane, 2 * LANES, LANES)):
            copy = pltpu.make_async_remote_copy(
                src_ref=send_ref.at[at, pl.ds(start, span)], dst_ref=out_ref.at[at, pl.ds(lane, span)],
                send_sem=ss.at[len(sent)], recv_sem=rs.at[len(sent)],
                device_id={"col": other}, device_id_type=MESH,
            )
            copy.start()
            sent.append(copy)

    packed = 0, 2 * LANES, LANES
    lax.fori_loop(0, block // PICK, picker(0, [(send_ref, 0, packed), (out_ref, 0, kept)]), 0)
    send(0, block)
    piece = columns // (SENDS - 1)
    for n in range(SENDS - 1):
        first = block + n * piece
        lax.fori_loop(0, piece // PICK, picker(first, [(send_ref, first, packed)]), 0)
        send(first, piece)
    lax.fori_loop(0, columns // PICK, picker(count, [(out_ref, block, kept)]), 0)
    for copy in sent:
        copy.wait()


def pair_coefficients(grid, table, sel, index, columns):
    planes, _, area = grid.shape
    own = sel.shape[0] // 2
    total = index.shape[2] * 8
    count = total - columns
    half = planes // 2 + 1
    whole = pl.BlockSpec(memory_space=pltpu.VMEM)
    assert 2 * own == TILES * LANES
    return pl.pallas_call(
        rho_kernel,
        out_shape=jax.ShapeDtypeStruct((count, 4 * own), jnp.bfloat16),
        in_specs=[pl.BlockSpec(memory_space=pl.ANY), whole, whole, whole],
        out_specs=whole,
        scratch_shapes=[
            pltpu.VMEM((planes, GROUP, area), jnp.float32),
            pltpu.VMEM((half, 2, GROUP, area), jnp.float32),
            pltpu.VMEM((half * RADIX, own, 2 * area // RADIX), jnp.bfloat16),
            pltpu.VMEM((half * area * TILES, LANES), jnp.float32),
            pltpu.VMEM((count, 2 * own), jnp.bfloat16),
            pltpu.SemaphoreType.DMA((2 * SENDS,)),
            pltpu.SemaphoreType.DMA((2 * SENDS,)),
            pltpu.SemaphoreType.DMA((9,)),
        ]
        + [pltpu.SMEM((1, index.shape[2]), jnp.int32)] * 9,
        compiler_params=pltpu.CompilerParams(vmem_limit_bytes=VMEM_BYTES, collective_id=2, has_side_effects=True),
        cost_estimate=pl.CostEstimate(flops=10**10, bytes_accessed=8 * 1024 * 1024, transcendentals=0),
        name="rho",
    )(index, sel, grid, table)


def gather_kernel(own_ref, out_ref, x_ref, zs, zr, ys, yr, cs, cr):
    row, col = lax.axis_index("row"), lax.axis_index("col")
    q, s = row // 2, row % 2
    lines = lax.axis_size("row") // 2
    peers = [lax.rem(q + d, lines) * 2 + s for d in range(1, lines)]
    pair, other = row + 1 - 2 * s, 1 - col
    for b in range(x_ref.shape[0]):
        x_ref[b] = own_ref[:, b, :].astype(x_ref.dtype)
    barrier = pltpu.get_barrier_semaphore()
    for target in [{"row": p} for p in peers] + [{"row": pair}, {"col": other}]:
        pl.semaphore_signal(barrier, inc=1, device_id=target, device_id_type=MESH)
    pl.semaphore_wait(barrier, lines + 1)
    sent = []

    def send(src, r, c, target, ssem, rsem):
        copy = pltpu.make_async_remote_copy(
            src_ref=src, dst_ref=out_ref.at[r, c], send_sem=ssem, recv_sem=rsem, device_id=target, device_id_type=MESH
        )
        copy.start()
        sent.append(copy)

    def arrived(r, c, ssem, rsem):
        pltpu.make_async_remote_copy(
            src_ref=x_ref, dst_ref=out_ref.at[r, c], send_sem=ssem, recv_sem=rsem,
            device_id={"col": other}, device_id_type=MESH,
        ).wait_recv()

    send(x_ref, row, col, {"row": pair}, ys.at[0], yr.at[0])
    order = sorted(range(1, lines), key=lambda d: min(d, lines - d))
    for d in order:
        send(x_ref, row, col, {"row": peers[d - 1]}, zs.at[d - 1], zr.at[d - 1])
    send(x_ref, row, col, {"col": other}, cs.at[0], cr.at[0])
    out_ref[row, col] = x_ref[...]
    for d in order:
        r = lax.rem(q + lines - d, lines) * 2 + s
        arrived(r, col, zs.at[d - 1], zr.at[d - 1])
        send(out_ref.at[r, col], r, col, {"row": pair}, ys.at[d], yr.at[d])
        send(out_ref.at[r, col], r, col, {"col": other}, cs.at[d], cr.at[d])
    for d in [0] + order:
        r = lax.rem(q + lines - d, lines) * 2 + 1 - s
        arrived(r, col, ys.at[d], yr.at[d])
        send(out_ref.at[r, col], r, col, {"col": other}, cs.at[lines + d], cr.at[lines + d])
    for d in range(lines):
        r = lax.rem(q + lines - d, lines) * 2
        arrived(r + s, other, cs.at[d], cr.at[d])
        arrived(r + 1 - s, other, cs.at[lines + d], cr.at[lines + d])
    for copy in sent:
        copy.wait_send()


def gather_planes(local):
    rows, cols = lax.axis_size("row"), lax.axis_size("col")
    lines = rows // 2
    shape = (local.shape[1], local.shape[0], local.shape[2])
    dma = pltpu.SemaphoreType.DMA
    whole = pl.BlockSpec(memory_space=pltpu.VMEM)
    got = pl.pallas_call(
        gather_kernel,
        out_shape=jax.ShapeDtypeStruct((rows, cols) + shape, jnp.bfloat16),
        in_specs=[whole],
        out_specs=whole,
        scratch_shapes=[pltpu.VMEM(shape, jnp.bfloat16)] + [dma((lines - 1,))] * 2 + [dma((lines,))] * 2 + [dma((2 * lines,))] * 2,
        compiler_params=pltpu.CompilerParams(collective_id=0, has_side_effects=True),
        name="planes",
    )(local)
    return got.reshape((-1,) + shape[1:])


def element_kernel(scale, w_ref, right_ref, out_ref, w, mixed, total, done, part, near, both, far, ws, ns, nr, fs, fr):
    count, lanes = right_ref.shape
    freqs, parts, depth, columns = w.shape
    block = count - columns
    stages, cols, rows, share, span = part.shape
    per = lanes // span
    pieces = ws.shape[1]
    tile = min(TILE, depth)
    tiles = depth // tile
    row, col = lax.axis_index("row"), lax.axis_index("col")
    other = 1 - col
    n, h = LANES, LANES // 2

    def load(f, i):
        at = pl.ds(pl.multiple_of(i * (depth // pieces), depth // pieces), depth // pieces)
        return pltpu.make_async_copy(w_ref.at[f, :, at], w.at[f, :, at], ws.at[f, i])

    for f in range(freqs):
        for i in range(pieces):
            load(f, i).start()

    barrier = pltpu.get_barrier_semaphore()
    for target in [{"row": lax.rem(row + d, rows)} for d in range(1, rows)] + [{"col": other}]:
        pl.semaphore_signal(barrier, inc=1, device_id=target, device_id_type=MESH)
    pl.semaphore_wait(barrier, rows)

    def to_pair(s):
        return pltpu.make_async_remote_copy(
            src_ref=part.at[s, other], dst_ref=near.at[s], send_sem=ns.at[s], recv_sem=nr.at[s],
            device_id={"col": other}, device_id_type=MESH,
        )

    def to_row(s, d):
        return pltpu.make_async_remote_copy(
            src_ref=both.at[s, d], dst_ref=far.at[s, d - 1], send_sem=fs.at[s, d - 1], recv_sem=fr.at[s, d - 1],
            device_id={"row": lax.rem(row + d, rows)}, device_id_type=MESH,
        )

    order = sorted(range(1, rows), key=lambda d: -min(d, rows - d))

    def pass_on(s):
        to_pair(s).wait_recv()
        for d in order + [0]:
            r = lax.rem(row + d, rows)
            both[s, d] = (part[s, col, r].astype(jnp.float32) + near[s, r].astype(jnp.float32)).astype(both.dtype)
        for d in order:
            to_row(s, d).start()

    low = lax.broadcasted_iota(jnp.int32, (1, n), 1) < h

    def tile_of(f, c, i):
        last = c == per - 1
        at_lanes = pl.ds(pl.multiple_of(c * span, span), span)
        at = slice(i * tile, (i + 1) * tile)
        real = jnp.dot(w[f, 0, at, :], right_ref[block:, at_lanes], preferred_element_type=jnp.float32)
        imag = jnp.dot(w[f, 1, at, :], right_ref[block:, at_lanes], preferred_element_type=jnp.float32)
        a, b = imag[:, :n], imag[:, n:]
        ra, rb = pltpu.roll(a, h, axis=1), pltpu.roll(b, h, axis=1)
        one = jnp.where(last, jnp.where(low, -ra, ra), -b)
        two = jnp.where(last, jnp.where(low, -rb, rb), a)
        mixed[at, :n] = ((real[:, :n] + one) * scale).astype(mixed.dtype)
        mixed[at, n:] = ((real[:, n:] + two) * scale).astype(mixed.dtype)

    def arrive(f, i):
        for j in range(pieces // tiles):
            load(f, i * (pieces // tiles) + j).wait()

    def stage(s, carry):
        f, c = s // per, s % per
        last = c == per - 1

        @pl.when(s == 0)
        def _():
            for i in range(tiles):
                arrive(0, i)
                tile_of(0, 0, i)

        @pl.when(s > 0)
        def _():
            @pl.when(c == 0)
            def _():
                for i in range(tiles):
                    arrive(f, i)

            for i in range(tiles):
                tile_of(f, c, i)
            pass_on(s - 1)

        total[...] = lax.dot_general(
            right_ref[:block, :], mixed[...], (((0,), (0,)), ((), ())), preferred_element_type=jnp.float32
        )
        for o in range(cols):
            own = lanes // 2 // cols
            for a0, p0, q0, size in ((0, 2 * n * o, 2 * n * o + n, n), (n, 4 * n + n * o, 4 * n + n * o + h, h)):
                ar, pr, qr = slice(o * own + a0, o * own + a0 + size), slice(p0, p0 + size), slice(q0, q0 + size)
                a, b = total[qr, :n], total[qr, n:]
                ra, rb = pltpu.roll(a, h, axis=1), pltpu.roll(b, h, axis=1)
                done[ar, :n] = total[pr, :n] + jnp.where(last, jnp.where(low, ra, -ra), b)
                done[ar, n:] = total[pr, n:] + jnp.where(last, jnp.where(low, rb, -rb), -a)
        for r in range(rows):
            for k in range(cols):
                d = (r * cols + k) * share
                part[s, k, r] = done[d : d + share, :].astype(part.dtype)
        to_pair(s).start()
        return carry

    lax.fori_loop(0, stages, stage, 0)
    pass_on(stages - 1)
    for s in range(stages):
        f, c = s // per, s % per
        summed = both[s, 0].astype(jnp.float32)
        for d in order[::-1]:
            to_row(s, d).wait_recv()
            summed += far[s, d - 1].astype(jnp.float32)
        x, y = summed[:, :n], summed[:, n:]
        if c < cols:
            at = c * (lanes // 2 // cols)
            out_ref[f, 0, :, at : at + n] = x
            out_ref[f, 1, :, at : at + n] = y
        else:
            for o, value in enumerate((x, y)):
                at = o * (lanes // 2 // cols) + n
                out_ref[f, 0, :, at : at + h] = value[:, :h]
                out_ref[f, 1, :, at : at + h] = value[:, h:]
    for s in range(stages):
        to_pair(s).wait_send()
        for d in order:
            to_row(s, d).wait_send()


def matrix_elements(screened, right, scale, tile=256):
    freqs, parts, depth, columns = screened.shape
    count, lanes = right.shape
    tile = min(tile, depth)
    members, cols = lax.axis_size("row"), lax.axis_size("col")
    pairs = lanes // 2
    share = pairs // (members * cols)
    span = 2 * LANES
    stages = freqs * lanes // span
    dma = pltpu.SemaphoreType.DMA
    whole = pl.BlockSpec(memory_space=pltpu.VMEM)
    piece = (share, span)
    return pl.pallas_call(
        functools.partial(element_kernel, scale),
        out_shape=jax.ShapeDtypeStruct((freqs, 2, share, pairs), jnp.float32),
        in_specs=[pl.BlockSpec(memory_space=pl.ANY), whole],
        out_specs=whole,
        scratch_shapes=[
            pltpu.VMEM(screened.shape, screened.dtype),
            pltpu.VMEM((depth, span), jnp.bfloat16),
            pltpu.VMEM((lanes, span), jnp.float32),
            pltpu.VMEM((pairs, span), jnp.float32),
            pltpu.VMEM((stages, cols, members) + piece, jnp.bfloat16),
            pltpu.VMEM((stages, members) + piece, jnp.bfloat16),
            pltpu.VMEM((stages, members) + piece, jnp.bfloat16),
            pltpu.VMEM((stages, members - 1) + piece, jnp.bfloat16),
            dma((freqs, depth // tile)),
            dma((stages,)),
            dma((stages,)),
            dma((stages, members - 1)),
            dma((stages, members - 1)),
        ],
        compiler_params=pltpu.CompilerParams(vmem_limit_bytes=ELEMENT_BYTES, collective_id=1, has_side_effects=True),
        cost_estimate=pl.CostEstimate(
            flops=8 * freqs * depth * columns * pairs, bytes_accessed=2 * screened.size, transcendentals=0
        ),
        name="elements",
    )(screened, right)


def plane_table(area):
    side = math.isqrt(area)
    inner = area // RADIX
    q = np.arange(RADIX).reshape(-1, 1, 1)
    k, n = np.arange(inner).reshape(1, -1, 1), np.arange(inner).reshape(1, 1, -1)
    turn = (q + RADIX * (k // side)) * (n // side) + (k % side) * (n % side)
    angle = (turn % side) * (2.0 * math.pi / side)
    c, s = np.cos(angle), np.sin(angle)
    both = np.concatenate([np.concatenate([c, s], axis=2), np.concatenate([-s, c], axis=2)], axis=1)
    return jnp.asarray(both.astype(jnp.bfloat16))


def shards(wannier, pairs, gmap, screened):
    functions, _, area = wannier.shape
    side = math.isqrt(area)
    count = pairs.shape[0]
    columns = screened.shape[3]
    block = screened.shape[2]
    row, col = lax.axis_index("row"), lax.axis_index("col")
    cols = lax.axis_size("col")
    own = count // cols

    grid = gather_planes(wannier)
    depth = grid.shape[0]

    mine = lax.dynamic_slice_in_dim(pairs, col * own, own, 0)
    mine = mine.reshape(own // GROUP, GROUP, 2).swapaxes(1, 2).reshape(-1, 1)
    sel = (mine == jnp.arange(functions, dtype=jnp.int32)[None, :]).astype(jnp.bfloat16)

    flat = jnp.concatenate(
        [
            lax.dynamic_slice_in_dim(gmap, row * block, block, 0),
            lax.dynamic_slice_in_dim(gmap, (1 - col) * columns, columns, 0),
            lax.dynamic_slice_in_dim(gmap, col * columns, columns, 0),
        ]
    )
    kx, ky, kz = flat // area, (flat // side) % side, flat % side
    far = kx > depth // 2
    kx = jnp.where(far, depth - kx, kx)
    ky = jnp.where(far, (side - ky) % side, ky)
    kz = jnp.where(far, (side - kz) % side, kz)
    cell = kx * area + (ky % RADIX) * (area // RADIX) + (ky // RADIX) * side + kz
    bits = jnp.sum(far.astype(jnp.int32).reshape(-1, PICK) << jnp.arange(PICK, dtype=jnp.int32), axis=1)
    bits = jnp.pad(bits, (0, cell.shape[0] // 8 - bits.shape[0]))
    index = jnp.concatenate([((cell // 8) * (8 * TILES) + cell % 8).reshape(-1, 8).T, bits[None, :]], axis=0)[:, None, :]

    right = pair_coefficients(grid, plane_table(area), sel, index, columns)
    scale = 1.0 / (depth * area * math.sqrt(gmap.shape[0]))
    return matrix_elements(screened, right, scale)


def solution(mesh):
    return jax.shard_map(
        shards,
        mesh=mesh,
        in_specs=(P("kpt", ("row", "col"), None), P(), P(), P("kpt", None, "row", "col")),
        out_specs=P(None, None, ("kpt", "row", "col"), None),
        check_vma=False,
    )
```
